128 devices in a mesh: data: 128 (over z, y, x, core).
Axes of the slice: x: 4, y: 4, z: 4, core: 2. Of those that a mesh axis runs over, the one named last changes fastest.
Arguments:
- act_in: bfloat16 [262144, 768], P('data')
- grad_out: bfloat16 [262144, 768], P('data')
- w_up: bfloat16 [2, 768, 2048], replicated
- w_down: bfloat16 [2, 2048, 768], replicated
- q_up: bfloat16 [2, 2048, 256], replicated
- q_down: bfloat16 [2, 768, 256], replicated
Outputs:
- output 1: bfloat16 [2, 768, 2048], replicated
- output 2: bfloat16 [2, 2048, 768], replicated
- output 3: float32 [2, 2048, 256], replicated
- output 4: float32 [2, 768, 256], replicated
All inputs are finite; a program needn't handle non-finite values.
Results may differ from the reference program's by a relative error of at most 0.0105384.
Values are sent between devices in bfloat16 or wider.
A program may use at most 1 GiB of HBM per device.

```python
import math
import jax
import jax.numpy as jnp
from jax import lax

DATA = 128
TOK = 2048
D = 768
FF = 2048
RANK = 256
LAYERS = 2

TOKENS = TOK * DATA
STEP_SIZE = 0.4 / math.sqrt(RANK)


def setup_inputs(seed: int = 0) -> dict:
    rng_key = jax.random.key(seed)
    sub_keys = jax.random.split(rng_key, 6)
    tok_rows = jax.random.normal(sub_keys[0], (TOKENS, D), jnp.float32)
    grad_rows = jax.random.normal(sub_keys[1], (TOKENS, D), jnp.float32) * (TOKENS ** -0.5)
    w_up = jax.random.normal(sub_keys[2], (LAYERS, D, FF), jnp.float32) * (D ** -0.5)
    w_down = jax.random.normal(sub_keys[3], (LAYERS, FF, D), jnp.float32) * (FF ** -0.5)
    q_up = jax.random.normal(sub_keys[4], (LAYERS, FF, RANK), jnp.float32) * (FF ** -0.5)
    q_down = jax.random.normal(sub_keys[5], (LAYERS, D, RANK), jnp.float32) * (D ** -0.5)
    return {"act_in": tok_rows.astype(jnp.bfloat16), "grad_out": grad_rows.astype(jnp.bfloat16), "w_up": w_up.astype(jnp.bfloat16), "w_down": w_down.astype(jnp.bfloat16), "q_up": q_up.astype(jnp.bfloat16), "q_down": q_down.astype(jnp.bfloat16)}


def gelu_tanh(values):
    return jax.nn.gelu(values, approximate=True)


def gelu_grad(pre_gelu, cot_gelu):
    pull_back = jax.vjp(gelu_tanh, pre_gelu)[1]
    return pull_back(cot_gelu)[0]


def mat_nn(left_op, right_op):
    return jnp.dot(left_op, right_op, preferred_element_type=jnp.float32)


def mat_nt(left_op, right_op):
    return lax.dot_general(left_op, right_op, (((1,), (1,)), ((), ())), preferred_element_type=jnp.float32)


def mat_tn(left_op, right_op):
    return lax.dot_general(left_op, right_op, (((0,), (0,)), ((), ())), preferred_element_type=jnp.float32)


def block_pairs(tok_rows, grad_rows, w_up, w_down):
    hiddens = []
    pre_gelus = []
    gelu_outs = []
    hidden = tok_rows
    for layer in range(LAYERS):
        hiddens.append(hidden)
        pre_gelu = mat_nn(hidden, w_up[layer]).astype(jnp.bfloat16)
        gelu_out = gelu_tanh(pre_gelu.astype(jnp.float32)).astype(jnp.bfloat16)
        pre_gelus.append(pre_gelu)
        gelu_outs.append(gelu_out)
        if layer + 1 < LAYERS:
            hidden = (hidden.astype(jnp.float32) + mat_nn(gelu_out, w_down[layer])).astype(jnp.bfloat16)
    up_pairs = [None] * LAYERS
    down_pairs = [None] * LAYERS
    cot_hidden = grad_rows
    for layer in reversed(range(LAYERS)):
        down_pairs[layer] = (gelu_outs[layer], cot_hidden)
        cot_gelu = mat_nt(cot_hidden, w_down[layer])
        cot_pre = gelu_grad(pre_gelus[layer].astype(jnp.float32), cot_gelu).astype(jnp.bfloat16)
        up_pairs[layer] = (hiddens[layer], cot_pre)
        if layer > 0:
            cot_hidden = (cot_hidden.astype(jnp.float32) + mat_nt(cot_pre, w_up[layer])).astype(jnp.bfloat16)
    return up_pairs, down_pairs


def left_term(row_pair, q_fac):
    left_in, right_in = row_pair
    sketch = mat_nn(right_in, q_fac).astype(jnp.bfloat16)
    return mat_tn(left_in, sketch)


def right_term(row_pair, p_hat):
    left_in, right_in = row_pair
    back_in = mat_nn(left_in, p_hat).astype(jnp.bfloat16)
    return mat_tn(right_in, back_in)


def col_normalise(p_sum):
    return (p_sum / jnp.sqrt(jnp.sum(p_sum * p_sum, axis=-2, keepdims=True))).astype(jnp.bfloat16)


def apply_update(weight, p_hat, q_sum):
    return (weight.astype(jnp.float32) - STEP_SIZE * mat_nt(p_hat, q_sum.astype(jnp.bfloat16))).astype(jnp.bfloat16)


def reference(act_in, grad_out, w_up, w_down, q_up, q_down):
    blocks = (act_in.reshape(DATA, TOK, D), grad_out.reshape(DATA, TOK, D))

    def left_pass(totals, block_pair):
        up_pairs, down_pairs = block_pairs(block_pair[0], block_pair[1], w_up, w_down)
        up_part = jnp.stack([left_term(up_pairs[layer], q_up[layer]) for layer in range(LAYERS)])
        down_part = jnp.stack([left_term(down_pairs[layer], q_down[layer]) for layer in range(LAYERS)])
        return (totals[0] + up_part, totals[1] + down_part), None

    left_zero = (jnp.zeros((LAYERS, D, RANK), jnp.float32), jnp.zeros((LAYERS, FF, RANK), jnp.float32))
    left_sums = lax.scan(left_pass, left_zero, blocks)[0]
    p_hat_up = col_normalise(left_sums[0])
    p_hat_down = col_normalise(left_sums[1])

    def right_pass(totals, block_pair):
        up_pairs, down_pairs = block_pairs(block_pair[0], block_pair[1], w_up, w_down)
        up_part = jnp.stack([right_term(up_pairs[layer], p_hat_up[layer]) for layer in range(LAYERS)])
        down_part = jnp.stack([right_term(down_pairs[layer], p_hat_down[layer]) for layer in range(LAYERS)])
        return (totals[0] + up_part, totals[1] + down_part), None

    right_zero = (jnp.zeros((LAYERS, FF, RANK), jnp.float32), jnp.zeros((LAYERS, D, RANK), jnp.float32))
    q_up_new, q_down_new = lax.scan(right_pass, right_zero, blocks)[0]
    w_up_new = jnp.stack([apply_update(w_up[layer], p_hat_up[layer], q_up_new[layer]) for layer in range(LAYERS)])
    w_down_new = jnp.stack([apply_update(w_down[layer], p_hat_down[layer], q_down_new[layer]) for layer in range(LAYERS)])
    return (w_up_new, w_down_new, q_up_new, q_down_new)
```

```python
import math
import functools
import jax
import jax.numpy as jnp
from jax import lax
from jax.experimental import pallas as pl
from jax.experimental.pallas import tpu as pltpu
from jax.sharding import PartitionSpec as P

MESH = pl.DeviceIdType.MESH
STRIDES = (2, 8, 32)
ORDERS = ((0, 1, 2), (1, 2, 0), (2, 0, 1))
COPIES = 47


def gelu_tanh(values):
    return jax.nn.gelu(values, approximate=True)


def gelu_grad(pre_gelu, cot_gelu):
    pull_back = jax.vjp(gelu_tanh, pre_gelu)[1]
    return pull_back(cot_gelu)[0]


def mat_nn(left_op, right_op):
    return jnp.dot(left_op, right_op, preferred_element_type=jnp.float32)


def mat_nt(left_op, right_op):
    return lax.dot_general(left_op, right_op, (((1,), (1,)), ((), ())), preferred_element_type=jnp.float32)


def mat_tn(left_op, right_op):
    return lax.dot_general(left_op, right_op, (((0,), (0,)), ((), ())), preferred_element_type=jnp.float32)


def block_pairs(tok_rows, grad_rows, w_up, w_down):
    layers = w_up.shape[0]
    hiddens = []
    pre_gelus = []
    gelu_outs = []
    hidden = tok_rows
    for layer in range(layers):
        hiddens.append(hidden)
        pre_gelu = mat_nn(hidden, w_up[layer]).astype(jnp.bfloat16)
        gelu_out = gelu_tanh(pre_gelu.astype(jnp.float32)).astype(jnp.bfloat16)
        pre_gelus.append(pre_gelu)
        gelu_outs.append(gelu_out)
        if layer + 1 < layers:
            hidden = (hidden.astype(jnp.float32) + mat_nn(gelu_out, w_down[layer])).astype(jnp.bfloat16)
    up_pairs = [None] * layers
    down_pairs = [None] * layers
    cot_hidden = grad_rows
    for layer in reversed(range(layers)):
        down_pairs[layer] = (gelu_outs[layer], cot_hidden)
        cot_gelu = mat_nt(cot_hidden, w_down[layer])
        cot_pre = gelu_grad(pre_gelus[layer].astype(jnp.float32), cot_gelu).astype(jnp.bfloat16)
        up_pairs[layer] = (hiddens[layer], cot_pre)
        if layer > 0:
            cot_hidden = (cot_hidden.astype(jnp.float32) + mat_nt(cot_pre, w_up[layer])).astype(jnp.bfloat16)
    return up_pairs, down_pairs


def flip(place, bit):
    if bit == 1:
        return place + 1 - 2 * lax.rem(place, 2)
    if bit == 2:
        return lax.rem(place + 2, 4)
    return 3 - place


def position(axis):
    me = lax.axis_index(axis)
    core = lax.rem(me, 2)
    places = tuple(lax.rem(lax.div(me, stride), 4) for stride in STRIDES)
    return me, core, places


def greet(pos):
    me, core, places = pos
    barrier = pltpu.get_barrier_semaphore()
    pl.semaphore_signal(barrier, inc=1, device_id=(me + 1 - 2 * core,), device_id_type=MESH)
    for dim in range(3):
        for bit in (1, 2, 3):
            peer = me + (flip(places[dim], bit) - places[dim]) * STRIDES[dim]
            pl.semaphore_signal(barrier, inc=1, device_id=(peer,), device_id_type=MESH)
    pl.semaphore_wait(barrier, 10)


class SumAll:
    def __init__(self, acc, bufs, sems, pos, lanes):
        self.acc, self.bufs, self.sems, self.pos = acc, bufs, sems, pos
        third = lanes // 3 // 128 * 128
        self.groups = ((0, third), (third, third), (2 * third, lanes - 2 * third))

    def rows(self, start, size, lo, width):
        return self.acc.at[pl.ds(pl.multiple_of(start, 8), size), pl.ds(lo, width)]

    def copies(self, phase):
        me, core, places = self.pos
        send, recv = self.sems[:2]
        lanes = self.acc.shape[1]
        out = []

        def add(index, src, dst, peer):
            out.append(pltpu.make_async_remote_copy(src_ref=src, dst_ref=dst, send_sem=send.at[index], recv_sem=recv.at[index], device_id=(peer,), device_id_type=MESH))

        partner = me + 1 - 2 * core
        if phase == 0:
            add(0, self.rows((1 - core) * 128, 128, 0, lanes), self.bufs[0], partner)
            return out
        if phase == 6:
            mine = self.rows(core * 128, 128, 0, lanes)
            add(46, mine, mine, partner)
            return out
        for group, (lo, width) in enumerate(self.groups):
            first, second, third = ORDERS[group]
            top = core * 128
            block = top + places[first] * 32
            base = block + places[second] * 8
            dim = {1: first, 2: second, 3: third, 4: second, 5: first}[phase]
            for bit in (1, 2, 3):
                other = flip(places[dim], bit)
                peer = me + (other - places[dim]) * STRIDES[dim]
                index = 1 + (phase - 1) * 9 + group * 3 + bit - 1
                if phase == 1:
                    src, dst = self.rows(top + other * 32, 32, lo, width), self.bufs[1].at[bit - 1, :, pl.ds(lo, width)]
                elif phase == 2:
                    src, dst = self.rows(block + other * 8, 8, lo, width), self.bufs[2].at[bit - 1, :, pl.ds(lo, width)]
                elif phase == 3:
                    src, dst = self.rows(base, 8, lo, width), self.bufs[3].at[bit - 1, :, pl.ds(lo, width)]
                elif phase == 4:
                    src = dst = self.rows(base, 8, lo, width)
                else:
                    src = dst = self.rows(block, 32, lo, width)
                add(index, src, dst, peer)
        return out

    def start(self, phase):
        if phase == 6:
            pl.semaphore_wait(self.sems[2], 1)
        for copy in self.copies(phase):
            copy.start()

    def finish(self, phase):
        for copy in self.copies(phase):
            copy.wait()
        me, core, places = self.pos
        if phase == 0:
            pl.semaphore_signal(self.sems[2], inc=1, device_id=(me + 1 - 2 * core,), device_id_type=MESH)
            mine = self.rows(core * 128, 128, 0, self.acc.shape[1])
            mine[...] += self.bufs[0][...]
            return
        if phase > 3:
            return
        for group, (lo, width) in enumerate(self.groups):
            first, second, third = ORDERS[group]
            block = core * 128 + places[first] * 32
            got = [self.bufs[phase][bit, :, pl.ds(lo, width)] for bit in range(3)]
            mine = self.rows(block, 32, lo, width) if phase == 1 else self.rows(block + places[second] * 8, 8, lo, width)
            mine[...] = (mine[...] + got[0]) + (got[1] + got[2])

    def step(self, phase):
        if phase > 0:
            self.finish(phase - 1)
        if phase < 7:
            self.start(phase)


def sum_kernel(axis, count, *refs):
    ins, outs, rest = refs[:count], refs[count:2 * count], refs[2 * count:]
    pos = position(axis)
    greet(pos)
    sums = []
    for k in range(count):
        outs[k][...] = ins[k][...]
        bufs, sems = rest[k * 7:k * 7 + 4], rest[k * 7 + 4:k * 7 + 7]
        sums.append(SumAll(outs[k], bufs, sems, pos, ins[k].shape[1]))
    for phase in range(8):
        for item in sums:
            item.step(phase)


def sum_scratch(lanes):
    return [pltpu.VMEM((128, lanes), jnp.float32), pltpu.VMEM((3, 32, lanes), jnp.float32), pltpu.VMEM((3, 8, lanes), jnp.float32), pltpu.VMEM((3, 8, lanes), jnp.float32), pltpu.SemaphoreType.DMA((COPIES,)), pltpu.SemaphoreType.DMA((COPIES,)), pltpu.SemaphoreType.REGULAR]


def sum_over_devices(arrays, axis, ident):
    scratch = []
    for array in arrays:
        scratch += sum_scratch(array.shape[1])
    return pl.pallas_call(
        functools.partial(sum_kernel, axis, len(arrays)),
        out_shape=[jax.ShapeDtypeStruct(a.shape, a.dtype) for a in arrays],
        in_specs=[pl.BlockSpec(memory_space=pltpu.VMEM)] * len(arrays),
        out_specs=[pl.BlockSpec(memory_space=pltpu.VMEM)] * len(arrays),
        scratch_shapes=scratch,
        compiler_params=pltpu.CompilerParams(collective_id=ident, has_side_effects=True, vmem_limit_bytes=40 * 2**20),
        name="sums" + str(ident),
    )(*arrays)


def solution(mesh):
    axis = mesh.axis_names[0]

    def local_step(tok_rows, grad_rows, w_up, w_down, q_up, q_down):
        step_size = 0.4 / math.sqrt(q_up.shape[-1])
        up_pairs, down_pairs = block_pairs(tok_rows, grad_rows, w_up, w_down)
        pairs = [down_pairs[1], up_pairs[1], down_pairs[0], up_pairs[0]]
        facs = [q_down[1], q_up[1], q_down[0], q_up[0]]
        weights = [w_down[1], w_up[1], w_down[0], w_up[0]]
        p_terms = []
        for (left, right), fac in zip(pairs, facs):
            sketch = mat_nn(right, fac).astype(jnp.bfloat16)
            p_terms.append(mat_tn(sketch, left))
        p_sums = sum_over_devices(p_terms, axis, 0)
        hats = [(p / jnp.sqrt(jnp.sum(p * p, axis=-1, keepdims=True))).astype(jnp.bfloat16) for p in p_sums]
        q_terms = []
        for (left, right), hat in zip(pairs, hats):
            back = mat_nt(left, hat).astype(jnp.bfloat16)
            q_terms.append(mat_tn(back, right))
        q_sums = sum_over_devices(q_terms, axis, 1)
        news = [(w.astype(jnp.float32) - step_size * mat_tn(hat, q.astype(jnp.bfloat16))).astype(jnp.bfloat16) for w, hat, q in zip(weights, hats, q_sums)]
        return jnp.stack([news[3], news[1]]), jnp.stack([news[2], news[0]]), jnp.stack([q_sums[3].T, q_sums[1].T]), jnp.stack([q_sums[2].T, q_sums[0].T])

    row_spec = P(axis, None)
    return jax.shard_map(local_step, mesh=mesh, in_specs=(row_spec, row_spec, P(), P(), P(), P()), out_specs=(P(), P(), P(), P()), check_vma=False)
```

```python
import math
import functools
import jax
import jax.numpy as jnp
from jax import lax
from jax.experimental import pallas as pl
from jax.experimental.pallas import tpu as pltpu
from jax.sharding import PartitionSpec as P

MESH = pl.DeviceIdType.MESH
STRIDES = (2, 8, 32)
ORDERS = ((0, 1, 2), (1, 2, 0), (2, 0, 1))
COPIES = 47


def mat_nn(left_op, right_op):
    return jnp.dot(left_op, right_op, preferred_element_type=jnp.float32)


def mat_nt(left_op, right_op):
    return lax.dot_general(left_op, right_op, (((1,), (1,)), ((), ())), preferred_element_type=jnp.float32)


def mat_tn(left_op, right_op):
    return lax.dot_general(left_op, right_op, (((0,), (0,)), ((), ())), preferred_element_type=jnp.float32)


def flip(place, bit):
    if bit == 1:
        return place + 1 - 2 * lax.rem(place, 2)
    if bit == 2:
        return lax.rem(place + 2, 4)
    return 3 - place


def position(axis):
    me = lax.axis_index(axis)
    core = lax.rem(me, 2)
    places = tuple(lax.rem(lax.div(me, stride), 4) for stride in STRIDES)
    return me, core, places


def greet(pos):
    me, core, places = pos
    barrier = pltpu.get_barrier_semaphore()
    pl.semaphore_signal(barrier, inc=1, device_id=(me + 1 - 2 * core,), device_id_type=MESH)
    for dim in range(3):
        for bit in (1, 2, 3):
            peer = me + (flip(places[dim], bit) - places[dim]) * STRIDES[dim]
            pl.semaphore_signal(barrier, inc=1, device_id=(peer,), device_id_type=MESH)
    pl.semaphore_wait(barrier, 10)


class SumAll:
    def __init__(self, acc, bufs, sems, pos, lanes):
        self.acc, self.bufs, self.sems, self.pos = acc, bufs, sems, pos
        third = lanes // 3 // 128 * 128
        self.groups = ((0, third), (third, third), (2 * third, lanes - 2 * third))

    def rows(self, start, size, lo, width):
        return self.acc.at[pl.ds(pl.multiple_of(start, 8), size), pl.ds(lo, width)]

    def copies(self, phase):
        me, core, places = self.pos
        send, recv = self.sems[:2]
        lanes = self.acc.shape[1]
        out = []

        def add(index, src, dst, peer):
            out.append(pltpu.make_async_remote_copy(src_ref=src, dst_ref=dst, send_sem=send.at[index], recv_sem=recv.at[index], device_id=(peer,), device_id_type=MESH))

        partner = me + 1 - 2 * core
        if phase == 0:
            add(0, self.rows((1 - core) * 128, 128, 0, lanes), self.bufs[0], partner)
            return out
        if phase == 6:
            mine = self.rows(core * 128, 128, 0, lanes)
            add(46, mine, mine, partner)
            return out
        for group, (lo, width) in enumerate(self.groups):
            first, second, third = ORDERS[group]
            top = core * 128
            block = top + places[first] * 32
            base = block + places[second] * 8
            dim = {1: first, 2: second, 3: third, 4: second, 5: first}[phase]
            for bit in (1, 2, 3):
                other = flip(places[dim], bit)
                peer = me + (other - places[dim]) * STRIDES[dim]
                index = 1 + (phase - 1) * 9 + group * 3 + bit - 1
                if phase == 1:
                    src, dst = self.rows(top + other * 32, 32, lo, width), self.bufs[1].at[bit - 1, :, pl.ds(lo, width)]
                elif phase == 2:
                    src, dst = self.rows(block + other * 8, 8, lo, width), self.bufs[2].at[bit - 1, :, pl.ds(lo, width)]
                elif phase == 3:
                    src, dst = self.rows(base, 8, lo, width), self.bufs[3].at[bit - 1, :, pl.ds(lo, width)]
                elif phase == 4:
                    src = dst = self.rows(base, 8, lo, width)
                else:
                    src = dst = self.rows(block, 32, lo, width)
                add(index, src, dst, peer)
        return out

    def start(self, phase):
        if phase == 6:
            pl.semaphore_wait(self.sems[2], 1)
        for copy in self.copies(phase):
            copy.start()

    def finish(self, phase):
        for copy in self.copies(phase):
            copy.wait()
        me, core, places = self.pos
        if phase == 0:
            pl.semaphore_signal(self.sems[2], inc=1, device_id=(me + 1 - 2 * core,), device_id_type=MESH)
            mine = self.rows(core * 128, 128, 0, self.acc.shape[1])
            mine[...] += self.bufs[0][...]
            return
        if phase > 3:
            return
        for group, (lo, width) in enumerate(self.groups):
            first, second, third = ORDERS[group]
            block = core * 128 + places[first] * 32
            got = [self.bufs[phase][bit, :, pl.ds(lo, width)] for bit in range(3)]
            mine = self.rows(block, 32, lo, width) if phase == 1 else self.rows(block + places[second] * 8, 8, lo, width)
            mine[...] = (mine[...] + got[0]) + (got[1] + got[2])

    def step(self, phase):
        if phase > 0:
            self.finish(phase - 1)
        if phase < 7:
            self.start(phase)


TILE = 256
LANES = 256
ROOT = math.sqrt(2.0 / math.pi)


def gelu(z):
    half = 0.5 * z
    return half + half * jnp.tanh(z * (ROOT + (ROOT * 0.044715) * (z * z)))


def gelu_slope(z):
    square = z * z
    t = jnp.tanh(z * (ROOT + (ROOT * 0.044715) * square))
    return (0.5 + 0.5 * t) + (0.5 * z) * (1.0 - t * t) * (ROOT + (3.0 * ROOT * 0.044715) * square)


def tile_rows(i):
    return pl.ds(pl.multiple_of(i * TILE, TILE), TILE)


def step_kernel(axis, *refs):
    (x_hbm, dy_hbm, wu_hbm, wd_hbm, qu_hbm, qd_hbm, hat_u_hbm, hat_d_hbm, sum_u_hbm, sum_d_hbm,
     a0, z0, a1, z1, h1, g1, wu, wd, qu, qd, trans, stream_buf, pd1, pu1, pd0, pu0, extra,
     stream_sem, load_sem, out_sem, *rest) = refs
    tiles = x_hbm.shape[0] // TILE
    bf16 = jnp.bfloat16
    f32 = jnp.float32
    channels = [rest[7 * k:7 * k + 7] for k in range(5)]

    def load(index, src, dst):
        return pltpu.make_async_copy(src, dst, load_sem.at[index])

    def tile_copy(src, i, slot):
        return pltpu.make_async_copy(src.at[tile_rows(i)], stream_buf.at[slot], stream_sem.at[slot])

    def loop(body, hooks=None):
        def run(i, carry):
            for when, hook in (hooks or {}).items():
                pl.when(i == when)(hook)
            body(i)
            return carry
        lax.fori_loop(0, tiles, run, 0)

    def streamed(src, following, body, hooks=None):
        def run(i):
            slot = lax.rem(i, 2)

            @pl.when(i + 1 < tiles)
            def _():
                tile_copy(src, i + 1, 1 - slot).start()
            tile_copy(src, i, slot).wait()
            body(i, stream_buf.at[slot])
        loop(run, hooks)
        if following is not None:
            tile_copy(following, 0, 0).start()

    tile_copy(x_hbm, 0, 0).start()
    load_wu0 = load(0, wu_hbm.at[0], wu)
    load_wd0 = load(1, wd_hbm.at[0], wd)
    load_qd1 = load(2, qd_hbm.at[1], qd)
    load_qu1 = load(3, qu_hbm.at[1], qu)
    load_wu1 = load(4, wu_hbm.at[1], wu)
    load_wd1 = load(5, wd_hbm.at[1], wd)
    load_wd0b = load(6, wd_hbm.at[0], wd)
    load_qd0 = load(7, qd_hbm.at[0], qd)
    load_qu0 = load(8, qu_hbm.at[0], qu)
    load_wu0.start()
    load_wd0.start()
    load_qd1.start()
    load_qu1.start()
    pos = position(axis)
    greet(pos)

    def reducer(acc, channel):
        return SumAll(acc, channels[channel][:4], channels[channel][4:], pos, acc.shape[1])

    d1, u1, d0, u0 = reducer(pd1, 0), reducer(pu1, 2), reducer(pd0, 1), reducer(pu0, 3)
    q_d1, q_u1, q_d0, q_u0 = reducer(pu1, 2), reducer(pd1, 0), reducer(extra, 4), reducer(pd0, 1)

    def up_rows(i, left, pre, post):
        for n in range(0, pre.shape[1], LANES):
            z = mat_nn(left, wu[:, n:n + LANES]).astype(bf16)
            pre[tile_rows(i), n:n + LANES] = z
            post[tile_rows(i), n:n + LANES] = gelu(z.astype(f32)).astype(bf16)

    def cot_rows(i, cot, pre):
        for n in range(0, pre.shape[1], LANES):
            c = mat_nt(cot, wd[n:n + LANES, :])
            z = pre[tile_rows(i), n:n + LANES].astype(f32)
            pre[tile_rows(i), n:n + LANES] = (gelu_slope(z) * c).astype(bf16)

    def put_trans(i, value):
        trans[:, tile_rows(i)] = value.T.astype(bf16)

    def full_product(acc, right):
        for n in range(0, acc.shape[1], 256):
            acc[:, n:n + 256] = mat_nn(trans[...], right[:, n:n + 256])

    def normalise(acc, out, row, index, dst):
        def run(k, carry):
            rows = pl.ds(pl.multiple_of(k * 32, 32), 32)
            p = acc[rows, :]
            out[pl.ds(pl.multiple_of(row + k * 32, 32), 32), :] = (p / jnp.sqrt(jnp.sum(p * p, axis=1, keepdims=True))).astype(bf16)
            return carry
        lax.fori_loop(0, 8, run, 0)
        pltpu.make_async_copy(out.at[row:row + 256], dst, out_sem.at[index]).start()

    def z0_stage(i, x_tile):
        up_rows(i, x_tile[...], z0, a0)

    load_wu0.wait()
    streamed(x_hbm, x_hbm, z0_stage)
    load_wu1.start()
    load_wd0.wait()

    def h1_stage(i, x_tile):
        for n in range(0, h1.shape[1], 256):
            h1[tile_rows(i), n:n + 256] = (x_tile[:, n:n + 256].astype(f32) + mat_nn(a0[tile_rows(i), :], wd[:, n:n + 256])).astype(bf16)
    streamed(x_hbm, dy_hbm, h1_stage)
    load_wd1.start()
    load_wu1.wait()
    loop(lambda i: up_rows(i, h1[tile_rows(i), :], z1, a1))
    load_qd1.wait()

    def sd1_stage(i, dy_tile):
        put_trans(i, mat_nn(dy_tile[...], qd[...]))
    streamed(dy_hbm, dy_hbm, sd1_stage)
    load_qd0.start()
    full_product(pd1, a1)
    d1.step(0)
    load_wd1.wait()
    load_qu1.wait()

    def e1_stage(i, dy_tile):
        cot_rows(i, dy_tile[...], z1)
        put_trans(i, mat_nn(z1[tile_rows(i), :], qu[...]))
    streamed(dy_hbm, dy_hbm, e1_stage, {1: lambda: d1.step(1), 3: lambda: d1.step(2)})
    load_wd0b.start()
    load_qu0.start()
    full_product(pu1, h1)
    u1.step(0)

    def g1_stage(i, dy_tile):
        for n in range(0, g1.shape[1], 256):
            g1[tile_rows(i), n:n + 256] = (dy_tile[:, n:n + 256].astype(f32) + mat_nt(z1[tile_rows(i), :], wu[n:n + 256, :])).astype(bf16)

    def g1_second():
        u1.step(1)
        d1.step(4)

    def g1_fourth():
        d1.step(5)
        u1.step(3)
    streamed(dy_hbm, x_hbm, g1_stage, {0: lambda: d1.step(3), 1: g1_second, 2: lambda: u1.step(2), 3: g1_fourth})
    load_qd0.wait()
    loop(lambda i: put_trans(i, mat_nn(g1[tile_rows(i), :], qd[...])), {2: lambda: u1.step(4)})
    full_product(pd0, a0)
    d0.step(0)
    d1.step(6)
    u1.step(5)
    load_wd0b.wait()
    load_qu0.wait()

    def e0_stage(i, x_tile):
        cot_rows(i, g1[tile_rows(i), :], z0)
        sketch = mat_nn(z0[tile_rows(i), :], qu[...]).T.astype(bf16)
        part = mat_nn(sketch, x_tile[...])

        @pl.when(i == 0)
        def _():
            pu0[...] = part

        @pl.when(i > 0)
        def _():
            pu0[...] += part

    def e0_second():
        d0.step(1)
        d1.step(7)
        u1.step(6)

    def e0_third():
        u1.step(7)
        normalise(pd1, wu, 0, 0, hat_d_hbm.at[1])
    streamed(x_hbm, dy_hbm, e0_stage, {1: e0_second, 2: e0_third, 3: lambda: d0.step(2)})
    u0.step(0)
    d0.step(3)
    normalise(pu1, wd, 0, 1, hat_u_hbm.at[1])

    def qd1_stage(i, dy_tile):
        back = mat_nt(a1[tile_rows(i), :], wu[0:256, :]).T.astype(bf16)
        part = mat_nn(back, dy_tile[...])

        @pl.when(i == 0)
        def _():
            pu1[...] = part

        @pl.when(i > 0)
        def _():
            pu1[...] += part
    streamed(dy_hbm, x_hbm, qd1_stage, {2: lambda: (u0.step(1), d0.step(4)) and None})
    q_d1.step(0)
    u0.step(2)
    loop(lambda i: put_trans(i, mat_nt(h1[tile_rows(i), :], wd[0:256, :])))
    d0.step(5)
    full_product(pd1, z1)
    q_u1.step(0)
    u0.step(3)
    q_d1.step(1)
    d0.step(6)
    u0.step(4)
    q_u1.step(1)
    d0.step(7)
    normalise(pd0, wu, 256, 2, hat_d_hbm.at[0])
    u0.step(5)
    q_d1.step(2)
    loop(lambda i: put_trans(i, mat_nt(a0[tile_rows(i), :], wu[256:512, :])), {2: lambda: (u0.step(6), q_u1.step(2)) and None})
    full_product(extra, g1)
    q_d0.step(0)
    q_d1.step(3)
    u0.step(7)
    normalise(pu0, wd, 256, 3, hat_u_hbm.at[0])
    q_u1.step(3)

    def uu0_stage(i, x_tile):
        put_trans(i, mat_nt(x_tile[...], wd[256:512, :]))
    streamed(x_hbm, None, uu0_stage)
    q_d1.step(4)
    q_d0.step(1)
    full_product(pd0, z0)
    q_u0.step(0)
    q_u1.step(4)
    q_d1.step(5)
    q_d0.step(2)
    q_u0.step(1)
    q_u1.step(5)
    q_d1.step(6)
    q_d0.step(3)
    q_u0.step(2)
    q_d1.step(7)
    q_u1.step(6)
    q_d0.step(4)
    q_u0.step(3)
    q_u1.step(7)
    q_d0.step(5)
    q_u0.step(4)
    q_d0.step(6)
    q_u0.step(5)
    q_d0.step(7)
    q_u0.step(6)
    q_u0.step(7)
    results = [(pu1, sum_d_hbm.at[1]), (pd1, sum_u_hbm.at[1]), (extra, sum_d_hbm.at[0]), (pd0, sum_u_hbm.at[0])]
    outs = [pltpu.make_async_copy(src, dst, out_sem.at[4 + k]) for k, (src, dst) in enumerate(results)]
    for copy in outs:
        copy.start()
    hats = [(wu, 0, hat_d_hbm.at[1]), (wd, 0, hat_u_hbm.at[1]), (wu, 256, hat_d_hbm.at[0]), (wd, 256, hat_u_hbm.at[0])]
    for k, (src, row, dst) in enumerate(hats):
        pltpu.make_async_copy(src.at[row:row + 256], dst, out_sem.at[k]).wait()
    for copy in outs:
        copy.wait()


def sum_scratch(lanes):
    return [pltpu.VMEM((128, lanes), jnp.float32), pltpu.VMEM((3, 32, lanes), jnp.float32), pltpu.VMEM((3, 8, lanes), jnp.float32), pltpu.VMEM((3, 8, lanes), jnp.float32), pltpu.SemaphoreType.DMA((COPIES,)), pltpu.SemaphoreType.DMA((COPIES,)), pltpu.SemaphoreType.REGULAR]


def power_sums(axis, tok_rows, grad_rows, w_up, w_down, q_up, q_down):
    tokens, model = tok_rows.shape
    layers, _, wide = w_up.shape
    rank = q_up.shape[-1]
    bf16, f32 = jnp.bfloat16, jnp.float32
    scratch = [pltpu.VMEM((tokens, wide), bf16)] * 4 + [pltpu.VMEM((tokens, model), bf16)] * 2
    scratch += [pltpu.VMEM((model, wide), bf16), pltpu.VMEM((wide, model), bf16), pltpu.VMEM((wide, rank), bf16), pltpu.VMEM((model, rank), bf16)]
    scratch += [pltpu.VMEM((rank, tokens), bf16), pltpu.VMEM((2, TILE, model), bf16)]
    scratch += [pltpu.VMEM((rank, lanes), f32) for lanes in (wide, model, wide, model, model)]
    scratch += [pltpu.SemaphoreType.DMA((2,)), pltpu.SemaphoreType.DMA((9,)), pltpu.SemaphoreType.DMA((8,))]
    for lanes in (wide, wide, model, model, model):
        scratch += sum_scratch(lanes)
    return pl.pallas_call(
        functools.partial(step_kernel, axis),
        out_shape=[jax.ShapeDtypeStruct((layers, rank, model), bf16), jax.ShapeDtypeStruct((layers, rank, wide), bf16), jax.ShapeDtypeStruct((layers, rank, wide), f32), jax.ShapeDtypeStruct((layers, rank, model), f32)],
        in_specs=[pl.BlockSpec(memory_space=pl.ANY)] * 6,
        out_specs=[pl.BlockSpec(memory_space=pl.ANY)] * 4,
        scratch_shapes=scratch,
        compiler_params=pltpu.CompilerParams(collective_id=0, has_side_effects=True, vmem_limit_bytes=67043328),
        name="power_sums",
    )(tok_rows, grad_rows, w_up, w_down, q_up, q_down)


def update_kernel(step_size, hat_u, hat_d, sum_u, sum_d, sum_u_part, sum_d_part, w_up, w_down, up_new, down_new, up_fac, down_fac):
    up_new[0] = (w_up[0].astype(jnp.float32) - step_size * mat_tn(hat_u[0], sum_u[0].astype(jnp.bfloat16))).astype(jnp.bfloat16)
    down_new[0] = (w_down[0].astype(jnp.float32) - step_size * mat_tn(hat_d[0], sum_d[0].astype(jnp.bfloat16))).astype(jnp.bfloat16)
    up_fac[0] = sum_u_part[0].T
    down_fac[0] = sum_d_part[0].T


def update(step_size, hat_u, hat_d, sum_u, sum_d, w_up, w_down):
    layers, model, wide = w_up.shape
    rank = hat_u.shape[1]
    parts = 2
    bf16, f32 = jnp.bfloat16, jnp.float32

    def cols(lanes):
        return pl.BlockSpec((1, rank, lanes // parts), lambda l, p: (l, 0, p))

    def whole(lanes):
        return pl.BlockSpec((1, rank, lanes), lambda l, p: (l, 0, 0))

    def rows(count, lanes):
        return pl.BlockSpec((1, count // parts, lanes), lambda l, p: (l, p, 0))

    return pl.pallas_call(
        functools.partial(update_kernel, step_size),
        grid=(layers, parts),
        in_specs=[cols(model), cols(wide), whole(wide), whole(model), cols(wide), cols(model), rows(model, wide), rows(wide, model)],
        out_specs=[rows(model, wide), rows(wide, model), rows(wide, rank), rows(model, rank)],
        out_shape=[jax.ShapeDtypeStruct((layers, model, wide), bf16), jax.ShapeDtypeStruct((layers, wide, model), bf16), jax.ShapeDtypeStruct((layers, wide, rank), f32), jax.ShapeDtypeStruct((layers, model, rank), f32)],
        compiler_params=pltpu.CompilerParams(vmem_limit_bytes=56 * 2**20),
        name="update",
    )(hat_u, hat_d, sum_u, sum_d, sum_u, sum_d, w_up, w_down)


def solution(mesh):
    axis = mesh.axis_names[0]

    def local_step(tok_rows, grad_rows, w_up, w_down, q_up, q_down):
        step_size = 0.4 / math.sqrt(q_up.shape[-1])
        hat_u, hat_d, sum_u, sum_d = power_sums(axis, tok_rows, grad_rows, w_up, w_down, q_up, q_down)
        return tuple(update(step_size, hat_u, hat_d, sum_u, sum_d, w_up, w_down))

    row_spec = P(axis, None)
    return jax.shard_map(local_step, mesh=mesh, in_specs=(row_spec, row_spec, P(), P(), P(), P()), out_specs=(P(), P(), P(), P()), check_vma=False)
```

```python
import math
import functools
import jax
import jax.numpy as jnp
from jax import lax
from jax.experimental import pallas as pl
from jax.experimental.pallas import tpu as pltpu
from jax.sharding import PartitionSpec as P

MESH = pl.DeviceIdType.MESH
STRIDES = (2, 8, 32)
ORDERS = ((0, 1, 2), (1, 2, 0), (2, 0, 1))
COPIES = 47


def mat_nn(left_op, right_op):
    return jnp.dot(left_op, right_op, preferred_element_type=jnp.float32)


def mat_nt(left_op, right_op):
    return lax.dot_general(left_op, right_op, (((1,), (1,)), ((), ())), preferred_element_type=jnp.float32)


def mat_tn(left_op, right_op):
    return lax.dot_general(left_op, right_op, (((0,), (0,)), ((), ())), preferred_element_type=jnp.float32)


def flip(place, bit):
    if bit == 1:
        return place + 1 - 2 * lax.rem(place, 2)
    if bit == 2:
        return lax.rem(place + 2, 4)
    return 3 - place


def position(axis):
    me = lax.axis_index(axis)
    core = lax.rem(me, 2)
    places = tuple(lax.rem(lax.div(me, stride), 4) for stride in STRIDES)
    return me, core, places


def greet(pos):
    me, core, places = pos
    barrier = pltpu.get_barrier_semaphore()
    pl.semaphore_signal(barrier, inc=1, device_id=(me + 1 - 2 * core,), device_id_type=MESH)
    for dim in range(3):
        for bit in (1, 2, 3):
            peer = me + (flip(places[dim], bit) - places[dim]) * STRIDES[dim]
            pl.semaphore_signal(barrier, inc=1, device_id=(peer,), device_id_type=MESH)
    pl.semaphore_wait(barrier, 10)


class SumAll:
    def __init__(self, acc, bufs, sems, pos, lanes):
        self.acc, self.bufs, self.sems, self.pos = acc, bufs, sems, pos
        third = lanes // 3 // 128 * 128
        self.groups = ((0, third), (third, third), (2 * third, lanes - 2 * third))

    def rows(self, start, size, lo, width):
        return self.acc.at[pl.ds(pl.multiple_of(start, 8), size), pl.ds(lo, width)]

    def copies(self, phase):
        me, core, places = self.pos
        send, recv = self.sems[:2]
        lanes = self.acc.shape[1]
        out = []

        def add(index, src, dst, peer):
            out.append(pltpu.make_async_remote_copy(src_ref=src, dst_ref=dst, send_sem=send.at[index], recv_sem=recv.at[index], device_id=(peer,), device_id_type=MESH))

        partner = me + 1 - 2 * core
        if phase == 0:
            add(0, self.rows((1 - core) * 128, 128, 0, lanes), self.bufs[0], partner)
            return out
        if phase == 6:
            mine = self.rows(core * 128, 128, 0, lanes)
            add(46, mine, mine, partner)
            return out
        for group, (lo, width) in enumerate(self.groups):
            first, second, third = ORDERS[group]
            top = core * 128
            block = top + places[first] * 32
            base = block + places[second] * 8
            dim = {1: first, 2: second, 3: third, 4: second, 5: first}[phase]
            for bit in (1, 2, 3):
                other = flip(places[dim], bit)
                peer = me + (other - places[dim]) * STRIDES[dim]
                index = 1 + (phase - 1) * 9 + group * 3 + bit - 1
                if phase == 1:
                    src, dst = self.rows(top + other * 32, 32, lo, width), self.bufs[1].at[bit - 1, :, pl.ds(lo, width)]
                elif phase == 2:
                    src, dst = self.rows(block + other * 8, 8, lo, width), self.bufs[2].at[bit - 1, :, pl.ds(lo, width)]
                elif phase == 3:
                    src, dst = self.rows(base, 8, lo, width), self.bufs[3].at[bit - 1, :, pl.ds(lo, width)]
                elif phase == 4:
                    src = dst = self.rows(base, 8, lo, width)
                else:
                    src = dst = self.rows(block, 32, lo, width)
                add(index, src, dst, peer)
        return out

    def start(self, phase):
        if phase == 6:
            pl.semaphore_wait(self.sems[2], 1)
        for copy in self.copies(phase):
            copy.start()

    def finish(self, phase):
        for copy in self.copies(phase):
            copy.wait()
        me, core, places = self.pos
        if phase == 0:
            pl.semaphore_signal(self.sems[2], inc=1, device_id=(me + 1 - 2 * core,), device_id_type=MESH)
            def add(k, carry):
                mine = self.rows(core * 128 + k * 8, 8, 0, self.acc.shape[1])
                mine[...] += self.bufs[0][pl.ds(pl.multiple_of(k * 8, 8), 8), :]
                return carry
            lax.fori_loop(0, 16, add, 0)
            return
        if phase > 3:
            return
        for group, (lo, width) in enumerate(self.groups):
            first, second, third = ORDERS[group]
            block = core * 128 + places[first] * 32
            for k in range(4 if phase == 1 else 1):
                got = [self.bufs[phase][bit, k * 8:k * 8 + 8, pl.ds(lo, width)] for bit in range(3)]
                mine = self.rows(block + k * 8 if phase == 1 else block + places[second] * 8, 8, lo, width)
                mine[...] = (mine[...] + got[0]) + (got[1] + got[2])

    def step(self, phase):
        if phase > 0:
            self.finish(phase - 1)
        if phase < 7:
            self.start(phase)


PLAN = {'e1_1': ('d1',),
 'e1_3': ('d1',),
 'pu1': ('d1',),
 'g1_1': ('u1', 'd1'),
 'g1_3': ('u1', 'd1'),
 'sd0_0': ('u1',),
 'e0_0': ('d1', 'u1'),
 'e0_1': ('d0', 'u1', 'd1', 'hd1'),
 'e0_3': ('d0', 'u1'),
 'hats1': ('u1', 'd0'),
 'qd1_1': ('u0',),
 'qd1_2': ('d0',),
 'uu1_0': ('u0', 'd0'),
 'uu1_2': ('qd1',),
 'qu1': ('u0',),
 'hd0': ('d0', 'qu1', 'qd1', 'u0', 'd0'),
 'hu0': ('qu1', 'qd1', 'u0', 'qu1', 'qd1', 'u0', 'qu1', 'u0', 'qd1'),
 'uu0_2': ('qu1', 'qd0'),
 'uu0_3': ('qd1',),
 'end': ('qd1', 'qu1', 'qu0', 'qd0', 'qu1', 'qu0', 'qd0', 'qu0', 'qd0', 'qu0', 'qd0', 'qu0', 'qd0', 'qd0', 'qu0', 'qu0')}
TILE = 512
LANES = 256
ROOT = math.sqrt(2.0 / math.pi)


def gelu(z):
    half = 0.5 * z
    return half + half * jnp.tanh(z * (ROOT + (ROOT * 0.044715) * (z * z)))


def gelu_slope(z):
    square = z * z
    t = jnp.tanh(z * (ROOT + (ROOT * 0.044715) * square))
    return (0.5 + 0.5 * t) + (0.5 * z) * (1.0 - t * t) * (ROOT + (3.0 * ROOT * 0.044715) * square)


def tile_rows(i):
    return pl.ds(pl.multiple_of(i * TILE, TILE), TILE)


def step_kernel(axis, *refs):
    (x_hbm, dy_hbm, wu_hbm, wd_hbm, qu_hbm, qd_hbm, hat_u_hbm, hat_d_hbm, sum_u_hbm, sum_d_hbm,
     a0, z0, a1, z1, h1, g1, wu, wd, qu, qd, trans, stream_buf, pd1, pu1, pd0, pu0,
     stream_sem, load_sem, out_sem, *rest) = refs
    tiles = x_hbm.shape[0] // TILE
    bf16 = jnp.bfloat16
    f32 = jnp.float32
    channels = [rest[7 * k:7 * k + 7] for k in range(4)]

    def load(index, src, dst):
        return pltpu.make_async_copy(src, dst, load_sem.at[index])

    def tile_copy(src, i, slot):
        return pltpu.make_async_copy(src.at[tile_rows(i)], stream_buf.at[slot], stream_sem.at[slot])

    def loop(body, hooks=None):
        def run(i, carry):
            for when, hook in (hooks or {}).items():
                pl.when(i == when)(hook)
            body(i)
            return carry
        lax.fori_loop(0, tiles, run, 0)

    def streamed(src, following, body, hooks=None):
        def run(i):
            slot = lax.rem(i, 2)

            @pl.when(i + 1 < tiles)
            def _():
                tile_copy(src, i + 1, 1 - slot).start()
            tile_copy(src, i, slot).wait()
            body(i, stream_buf.at[slot])
        loop(run, hooks)
        if following is not None:
            tile_copy(following, 0, 0).start()

    tile_copy(x_hbm, 0, 0).start()
    load_wu0 = load(0, wu_hbm.at[0], wu)
    load_wd0 = load(1, wd_hbm.at[0], wd)
    load_qd1 = load(2, qd_hbm.at[1], qd)
    load_qu1 = load(3, qu_hbm.at[1], qu)
    load_wu1 = load(4, wu_hbm.at[1], wu)
    load_wd1 = load(5, wd_hbm.at[1], wd)
    load_wd0b = load(6, wd_hbm.at[0], wd)
    load_qd0 = load(7, qd_hbm.at[0], qd)
    load_qu0 = load(8, qu_hbm.at[0], qu)
    load_wu0.start()
    load_wd0.start()
    load_qd1.start()
    load_qu1.start()
    pos = position(axis)
    greet(pos)

    def reducer(acc, channel):
        return SumAll(acc, channels[channel][:4], channels[channel][4:], pos, acc.shape[1])

    places = {"d1": (pd1, 0), "u1": (pu1, 2), "d0": (pd0, 1), "u0": (pu0, 3), "qd1": (pu1, 2), "qu1": (pd1, 0), "qd0": (pu0, 3), "qu0": (pd0, 1)}
    sums = {name: reducer(*place) for name, place in places.items()}
    phases = dict.fromkeys(places, 0)

    def act(key):
        for name in PLAN.get(key, ()):
            if name == "hd1":
                normalise(pd1, wu, 0, 0, hat_d_hbm.at[1])
            else:
                advance(name)

    def advance(name):
        sums[name].step(phases[name])
        phases[name] += 1

    def hooks(stage):
        return {i: functools.partial(act, stage + str(i)) for i in range(4) if PLAN.get(stage + str(i))}

    def up_rows(i, left, pre, post):
        for n in range(0, pre.shape[1], LANES):
            z = mat_nn(left, wu[:, n:n + LANES]).astype(bf16)
            pre[tile_rows(i), n:n + LANES] = z
            post[tile_rows(i), n:n + LANES] = gelu(z.astype(f32)).astype(bf16)

    def cot_rows(i, cot, pre):
        for n in range(0, pre.shape[1], LANES):
            c = mat_nt(cot, wd[n:n + LANES, :])
            z = pre[tile_rows(i), n:n + LANES].astype(f32)
            pre[tile_rows(i), n:n + LANES] = (gelu_slope(z) * c).astype(bf16)

    def put_trans(i, value):
        trans[:, tile_rows(i)] = value.T.astype(bf16)

    def full_product(acc, right):
        for n in range(0, acc.shape[1], 256):
            acc[:, n:n + 256] = mat_nn(trans[...], right[:, n:n + 256])

    def add_product(i, acc, left, right):
        @pl.when(i == 0)
        def _():
            acc[...] = jnp.zeros_like(acc)
        for n in range(0, acc.shape[1], 256):
            acc[:, n:n + 256] += mat_nn(left, right[:, n:n + 256])

    def normalise(acc, out, row, index, dst):
        def run(k, carry):
            rows = pl.ds(pl.multiple_of(k * 32, 32), 32)
            p = acc[rows, :]
            out[pl.ds(pl.multiple_of(row + k * 32, 32), 32), :] = (p / jnp.sqrt(jnp.sum(p * p, axis=1, keepdims=True))).astype(bf16)
            return carry
        lax.fori_loop(0, 8, run, 0)
        pltpu.make_async_copy(out.at[row:row + 256], dst, out_sem.at[index]).start()

    def z0_stage(i, x_tile):
        up_rows(i, x_tile[...], z0, a0)

    load_wu0.wait()
    streamed(x_hbm, x_hbm, z0_stage)
    load_wu1.start()
    load_wd0.wait()

    def h1_stage(i, x_tile):
        for n in range(0, h1.shape[1], 256):
            h1[tile_rows(i), n:n + 256] = (x_tile[:, n:n + 256].astype(f32) + mat_nn(a0[tile_rows(i), :], wd[:, n:n + 256])).astype(bf16)
    streamed(x_hbm, dy_hbm, h1_stage)
    load_wd1.start()
    load_wu1.wait()
    loop(lambda i: up_rows(i, h1[tile_rows(i), :], z1, a1))
    load_qd1.wait()

    def sd1_stage(i, dy_tile):
        put_trans(i, mat_nn(dy_tile[...], qd[...]))
    streamed(dy_hbm, dy_hbm, sd1_stage)
    load_qd0.start()
    full_product(pd1, a1)
    advance("d1")
    load_wd1.wait()
    load_qu1.wait()

    def e1_stage(i, dy_tile):
        cot_rows(i, dy_tile[...], z1)
        put_trans(i, mat_nn(z1[tile_rows(i), :], qu[...]))
    streamed(dy_hbm, dy_hbm, e1_stage, hooks("e1_"))
    load_wd0b.start()
    load_qu0.start()
    act("pu1")
    full_product(pu1, h1)
    advance("u1")

    def g1_stage(i, dy_tile):
        for n in range(0, g1.shape[1], 256):
            g1[tile_rows(i), n:n + 256] = (dy_tile[:, n:n + 256].astype(f32) + mat_nt(z1[tile_rows(i), :], wu[n:n + 256, :])).astype(bf16)
    streamed(dy_hbm, x_hbm, g1_stage, hooks("g1_"))
    load_qd0.wait()
    loop(lambda i: put_trans(i, mat_nn(g1[tile_rows(i), :], qd[...])), hooks("sd0_"))
    act("pd0")
    full_product(pd0, a0)
    advance("d0")
    load_wd0b.wait()
    load_qu0.wait()

    def e0_stage(i, x_tile):
        cot_rows(i, g1[tile_rows(i), :], z0)
        sketch = mat_nn(z0[tile_rows(i), :], qu[...]).T.astype(bf16)
        add_product(i, pu0, sketch, x_tile)
    streamed(x_hbm, dy_hbm, e0_stage, hooks("e0_"))
    advance("u0")
    act("hats1")
    normalise(pu1, wd, 0, 1, hat_u_hbm.at[1])

    def qd1_stage(i, dy_tile):
        back = mat_nt(a1[tile_rows(i), :], wu[0:256, :]).T.astype(bf16)
        add_product(i, pu1, back, dy_tile)
    streamed(dy_hbm, x_hbm, qd1_stage, hooks("qd1_"))
    advance("qd1")
    loop(lambda i: put_trans(i, mat_nt(h1[tile_rows(i), :], wd[0:256, :])), hooks("uu1_"))
    act("qu1")
    full_product(pd1, z1)
    advance("qu1")
    act("hd0")
    normalise(pd0, wu, 256, 2, hat_d_hbm.at[0])
    loop(lambda i: put_trans(i, mat_nt(a0[tile_rows(i), :], wu[256:512, :])), hooks("ud0_"))
    act("hu0")
    normalise(pu0, wd, 256, 3, hat_u_hbm.at[0])
    full_product(pu0, g1)
    advance("qd0")

    def uu0_stage(i, x_tile):
        put_trans(i, mat_nt(x_tile[...], wd[256:512, :]))
    streamed(x_hbm, None, uu0_stage, hooks("uu0_"))
    act("qu0")
    full_product(pd0, z0)
    advance("qu0")
    act("end")
    assert set(phases.values()) == {8}
    results = [(pu1, sum_d_hbm.at[1]), (pd1, sum_u_hbm.at[1]), (pu0, sum_d_hbm.at[0]), (pd0, sum_u_hbm.at[0])]
    outs = [pltpu.make_async_copy(src, dst, out_sem.at[4 + k]) for k, (src, dst) in enumerate(results)]
    for copy in outs:
        copy.start()
    hats = [(wu, 0, hat_d_hbm.at[1]), (wd, 0, hat_u_hbm.at[1]), (wu, 256, hat_d_hbm.at[0]), (wd, 256, hat_u_hbm.at[0])]
    for k, (src, row, dst) in enumerate(hats):
        pltpu.make_async_copy(src.at[row:row + 256], dst, out_sem.at[k]).wait()
    for copy in outs:
        copy.wait()


def sum_scratch(lanes):
    return [pltpu.VMEM((128, lanes), jnp.float32), pltpu.VMEM((3, 32, lanes), jnp.float32), pltpu.VMEM((3, 8, lanes), jnp.float32), pltpu.VMEM((3, 8, lanes), jnp.float32), pltpu.SemaphoreType.DMA((COPIES,)), pltpu.SemaphoreType.DMA((COPIES,)), pltpu.SemaphoreType.REGULAR]


def power_sums(axis, tok_rows, grad_rows, w_up, w_down, q_up, q_down):
    tokens, model = tok_rows.shape
    layers, _, wide = w_up.shape
    rank = q_up.shape[-1]
    bf16, f32 = jnp.bfloat16, jnp.float32
    scratch = [pltpu.VMEM((tokens, wide), bf16)] * 4 + [pltpu.VMEM((tokens, model), bf16)] * 2
    scratch += [pltpu.VMEM((model, wide), bf16), pltpu.VMEM((wide, model), bf16), pltpu.VMEM((wide, rank), bf16), pltpu.VMEM((model, rank), bf16)]
    scratch += [pltpu.VMEM((rank, tokens), bf16), pltpu.VMEM((2, TILE, model), bf16)]
    scratch += [pltpu.VMEM((rank, lanes), f32) for lanes in (wide, model, wide, model)]
    scratch += [pltpu.SemaphoreType.DMA((2,)), pltpu.SemaphoreType.DMA((9,)), pltpu.SemaphoreType.DMA((8,))]
    for lanes in (wide, wide, model, model):
        scratch += sum_scratch(lanes)
    return pl.pallas_call(
        functools.partial(step_kernel, axis),
        out_shape=[jax.ShapeDtypeStruct((layers, rank, model), bf16), jax.ShapeDtypeStruct((layers, rank, wide), bf16), jax.ShapeDtypeStruct((layers, rank, wide), f32), jax.ShapeDtypeStruct((layers, rank, model), f32)],
        in_specs=[pl.BlockSpec(memory_space=pl.ANY)] * 6,
        out_specs=[pl.BlockSpec(memory_space=pl.ANY)] * 4,
        scratch_shapes=scratch,
        compiler_params=pltpu.CompilerParams(collective_id=0, has_side_effects=True, vmem_limit_bytes=67043328),
        name="power_sums",
    )(tok_rows, grad_rows, w_up, w_down, q_up, q_down)


def update_kernel(step_size, hat_u, hat_d, sum_u, sum_d, w_up, w_down, up_new, down_new, up_fac, down_fac):
    up_new[0] = (w_up[0].astype(jnp.float32) - step_size * mat_tn(hat_u[0], sum_u[0].astype(jnp.bfloat16))).astype(jnp.bfloat16)
    down_new[0] = (w_down[0].astype(jnp.float32) - step_size * mat_tn(hat_d[0], sum_d[0].astype(jnp.bfloat16))).astype(jnp.bfloat16)
    up_fac[0] = sum_u[0].T

    @pl.when(pl.program_id(1) == 0)
    def _():
        down_fac[0] = sum_d[0].T


def update(step_size, hat_u, hat_d, sum_u, sum_d, w_up, w_down):
    layers, model, wide = w_up.shape
    rank = hat_u.shape[1]
    parts = 4
    part = wide // parts
    bf16, f32 = jnp.bfloat16, jnp.float32

    def cols(count):
        return pl.BlockSpec((1, count, part), lambda l, p: (l, 0, p))

    def rows(lanes):
        return pl.BlockSpec((1, part, lanes), lambda l, p: (l, p, 0))

    def whole(count, lanes):
        return pl.BlockSpec((1, count, lanes), lambda l, p: (l, 0, 0))

    return pl.pallas_call(
        functools.partial(update_kernel, step_size),
        grid=(layers, parts),
        in_specs=[whole(rank, model), cols(rank), cols(rank), whole(rank, model), cols(model), rows(model)],
        out_specs=[cols(model), rows(model), rows(rank), whole(model, rank)],
        out_shape=[jax.ShapeDtypeStruct((layers, model, wide), bf16), jax.ShapeDtypeStruct((layers, wide, model), bf16), jax.ShapeDtypeStruct((layers, wide, rank), f32), jax.ShapeDtypeStruct((layers, model, rank), f32)],
        compiler_params=pltpu.CompilerParams(vmem_limit_bytes=56 * 2**20),
        name="update",
    )(hat_u, hat_d, sum_u, sum_d, w_up, w_down)


def solution(mesh):
    axis = mesh.axis_names[0]

    def local_step(tok_rows, grad_rows, w_up, w_down, q_up, q_down):
        step_size = 0.4 / math.sqrt(q_up.shape[-1])
        hat_u, hat_d, sum_u, sum_d = power_sums(axis, tok_rows, grad_rows, w_up, w_down, q_up, q_down)
        return tuple(update(step_size, hat_u, hat_d, sum_u, sum_d, w_up, w_down))

    row_spec = P(axis, None)
    return jax.shard_map(local_step, mesh=mesh, in_specs=(row_spec, row_spec, P(), P(), P(), P()), out_specs=(P(), P(), P(), P()), check_vma=False)
```

```python
import math
import functools
import jax
import jax.numpy as jnp
from jax import lax
from jax.experimental import pallas as pl
from jax.experimental.pallas import tpu as pltpu
from jax.sharding import PartitionSpec as P

MESH = pl.DeviceIdType.MESH
STRIDES = (2, 8, 32)
ORDERS = ((0, 1, 2), (1, 2, 0), (2, 0, 1))
COPIES = 47


def mat_nn(left_op, right_op):
    return jnp.dot(left_op, right_op, preferred_element_type=jnp.float32)


def mat_nt(left_op, right_op):
    return lax.dot_general(left_op, right_op, (((1,), (1,)), ((), ())), preferred_element_type=jnp.float32)


def mat_tn(left_op, right_op):
    return lax.dot_general(left_op, right_op, (((0,), (0,)), ((), ())), preferred_element_type=jnp.float32)


def flip(place, bit):
    if bit == 1:
        return place + 1 - 2 * lax.rem(place, 2)
    if bit == 2:
        return lax.rem(place + 2, 4)
    return 3 - place


def position(axis):
    me = lax.axis_index(axis)
    core = lax.rem(me, 2)
    places = tuple(lax.rem(lax.div(me, stride), 4) for stride in STRIDES)
    return me, core, places


def greet(pos):
    me, core, places = pos
    barrier = pltpu.get_barrier_semaphore()
    pl.semaphore_signal(barrier, inc=1, device_id=(me + 1 - 2 * core,), device_id_type=MESH)
    for dim in range(3):
        for bit in (1, 2, 3):
            peer = me + (flip(places[dim], bit) - places[dim]) * STRIDES[dim]
            pl.semaphore_signal(barrier, inc=1, device_id=(peer,), device_id_type=MESH)
    pl.semaphore_wait(barrier, 10)


class SumAll:
    def __init__(self, acc, bufs, sems, pos, lanes):
        self.acc, self.bufs, self.sems, self.pos = acc, bufs, sems, pos
        third = lanes // 3 // 128 * 128
        self.groups = ((0, third), (third, third), (2 * third, lanes - 2 * third))

    def rows(self, start, size, lo, width):
        return self.acc.at[pl.ds(pl.multiple_of(start, 8), size), pl.ds(lo, width)]

    def copies(self, phase):
        me, core, places = self.pos
        send, recv = self.sems[:2]
        lanes = self.acc.shape[1]
        out = []

        def add(index, src, dst, peer):
            out.append(pltpu.make_async_remote_copy(src_ref=src, dst_ref=dst, send_sem=send.at[index], recv_sem=recv.at[index], device_id=(peer,), device_id_type=MESH))

        partner = me + 1 - 2 * core
        if phase == 0:
            add(0, self.rows((1 - core) * 128, 128, 0, lanes), self.bufs[0], partner)
            return out
        if phase == 6:
            mine = self.rows(core * 128, 128, 0, lanes)
            add(46, mine, mine, partner)
            return out
        for group, (lo, width) in enumerate(self.groups):
            first, second, third = ORDERS[group]
            top = core * 128
            block = top + places[first] * 32
            base = block + places[second] * 8
            dim = {1: first, 2: second, 3: third, 4: second, 5: first}[phase]
            for bit in (1, 2, 3):
                other = flip(places[dim], bit)
                peer = me + (other - places[dim]) * STRIDES[dim]
                index = 1 + (phase - 1) * 9 + group * 3 + bit - 1
                if phase == 1:
                    src, dst = self.rows(top + other * 32, 32, lo, width), self.bufs[1].at[bit - 1, :, pl.ds(lo, width)]
                elif phase == 2:
                    src, dst = self.rows(block + other * 8, 8, lo, width), self.bufs[2].at[bit - 1, :, pl.ds(lo, width)]
                elif phase == 3:
                    src, dst = self.rows(base, 8, lo, width), self.bufs[3].at[bit - 1, :, pl.ds(lo, width)]
                elif phase == 4:
                    src = dst = self.rows(base, 8, lo, width)
                else:
                    src = dst = self.rows(block, 32, lo, width)
                add(index, src, dst, peer)
        return out

    def start(self, phase):
        if phase == 6:
            pl.semaphore_wait(self.sems[2], 1)
        for copy in self.copies(phase):
            copy.start()

    def finish(self, phase):
        for copy in self.copies(phase):
            copy.wait()
        me, core, places = self.pos
        if phase == 0:
            pl.semaphore_signal(self.sems[2], inc=1, device_id=(me + 1 - 2 * core,), device_id_type=MESH)
            def add(k, carry):
                mine = self.rows(core * 128 + k * 8, 8, 0, self.acc.shape[1])
                mine[...] += self.bufs[0][pl.ds(pl.multiple_of(k * 8, 8), 8), :]
                return carry
            lax.fori_loop(0, 16, add, 0)
            return
        if phase > 3:
            return
        for group, (lo, width) in enumerate(self.groups):
            first, second, third = ORDERS[group]
            block = core * 128 + places[first] * 32
            for k in range(4 if phase == 1 else 1):
                got = [self.bufs[phase][bit, k * 8:k * 8 + 8, pl.ds(lo, width)] for bit in range(3)]
                mine = self.rows(block + k * 8 if phase == 1 else block + places[second] * 8, 8, lo, width)
                mine[...] = (mine[...] + got[0]) + (got[1] + got[2])

    def step(self, phase):
        if phase > 0:
            self.finish(phase - 1)
        if phase < 7:
            self.start(phase)


PLAN = {'e1_1': ('d1',),
 'pu1': ('d1',),
 'g1_2': ('u1', 'd1'),
 'sd0_1': ('d1', 'u1'),
 'e0_1': ('d1', 'u1', 'd0'),
 'e0_3': ('d1', 'u1'),
 'hats1': ('d0', 'd1', 'u1', 'u0', 'u1', 'd0', 'u1', 'u0', 'd0', 'hd1'),
 'qd1_1': ('u0',),
 'qd1_2': ('d0',),
 'qd1_3': ('u0',),
 'qu1': ('qd1', 'd0'),
 'qu1m': ('u0',),
 'hd0': ('d0',),
 'hu0': ('u0', 'qd1', 'qu1', 'u0'),
 'uu0_2': ('qd1',),
 'ud0_0': ('qd1', 'qu1'),
 'qd0': ('qu0',),
 'end': ('qd1',
         'qu1',
         'qd0',
         'qd1',
         'qu0',
         'qu1',
         'qd1',
         'qd0',
         'qu0',
         'qu1',
         'qd0',
         'qu0',
         'qu1',
         'qd0',
         'qu0',
         'qu1',
         'qd0',
         'qu0',
         'qd0',
         'qu0',
         'qd0')}
TILE = 512
LANES = 256
ROOT = math.sqrt(2.0 / math.pi)


def gelu(z):
    half = 0.5 * z
    return half + half * jnp.tanh(z * (ROOT + (ROOT * 0.044715) * (z * z)))


def gelu_slope(z):
    square = z * z
    t = jnp.tanh(z * (ROOT + (ROOT * 0.044715) * square))
    more = 1.0 + t
    return 0.5 * more + (more * z) * ((1.0 - t) * (0.5 * ROOT + (1.5 * ROOT * 0.044715) * square))


def tile_rows(i):
    return pl.ds(pl.multiple_of(i * TILE, TILE), TILE)


def step_kernel(axis, *refs):
    (x_hbm, dy_hbm, wu_hbm, wd_hbm, qu_hbm, qd_hbm, hat_u_hbm, hat_d_hbm, sum_u_hbm, sum_d_hbm,
     a0, z0, a1, z1, h1, g1, wu, wd, qu, qd, trans, stream_buf, pd1, pu1, pd0, pu0,
     stream_sem, load_sem, out_sem, *rest) = refs
    tiles = x_hbm.shape[0] // TILE
    bf16 = jnp.bfloat16
    f32 = jnp.float32
    channels = [rest[7 * k:7 * k + 7] for k in range(4)]

    def load(index, src, dst):
        return pltpu.make_async_copy(src, dst, load_sem.at[index])

    def tile_copy(src, i, slot):
        return pltpu.make_async_copy(src.at[tile_rows(i)], stream_buf.at[slot], stream_sem.at[slot])

    def loop(body, hooks=None):
        def run(i, carry):
            for when, hook in (hooks or {}).items():
                pl.when(i == when)(hook)
            body(i)
            return carry
        lax.fori_loop(0, tiles, run, 0)

    def streamed(src, following, body, hooks=None):
        def run(i):
            slot = lax.rem(i, 2)

            @pl.when(i + 1 < tiles)
            def _():
                tile_copy(src, i + 1, 1 - slot).start()
            tile_copy(src, i, slot).wait()
            body(i, stream_buf.at[slot])
        loop(run, hooks)
        if following is not None:
            tile_copy(following, 0, 0).start()

    tile_copy(x_hbm, 0, 0).start()
    load_wu0 = load(0, wu_hbm.at[0], wu)
    load_wd0 = load(1, wd_hbm.at[0], wd)
    load_qd1 = load(2, qd_hbm.at[1], qd)
    load_qu1 = load(3, qu_hbm.at[1], qu)
    load_wu1 = load(4, wu_hbm.at[1], wu)
    load_wd1 = load(5, wd_hbm.at[1], wd)
    load_wd0b = load(6, wd_hbm.at[0], wd)
    load_qd0 = load(7, qd_hbm.at[0], qd)
    load_qu0 = load(8, qu_hbm.at[0], qu)
    load_wu0.start()
    load_wd0.start()
    load_qd1.start()
    load_qu1.start()
    pos = position(axis)
    greet(pos)

    def reducer(acc, channel):
        return SumAll(acc, channels[channel][:4], channels[channel][4:], pos, acc.shape[1])

    places = {"d1": (pd1, 0), "u1": (pu1, 2), "d0": (pd0, 1), "u0": (pu0, 3), "qd1": (pu1, 2), "qu1": (pd1, 0), "qd0": (pu0, 3), "qu0": (pd0, 1)}
    sums = {name: reducer(*place) for name, place in places.items()}
    phases = dict.fromkeys(places, 0)
    spots = {"qd1": sum_d_hbm.at[1], "qu1": sum_u_hbm.at[1], "qd0": sum_d_hbm.at[0], "qu0": sum_u_hbm.at[0]}
    outs = {name: pltpu.make_async_copy(places[name][0], spot, out_sem.at[4 + k]) for k, (name, spot) in enumerate(spots.items())}

    def act(key):
        for name in PLAN.get(key, ()):
            if name == "hd1":
                normalise(pd1, wu, 0, 0, hat_d_hbm.at[1])
            else:
                advance(name)

    def advance(name):
        sums[name].step(phases[name])
        phases[name] += 1
        if phases[name] == 8 and name in outs:
            outs[name].start()

    def hooks(stage):
        return {i: functools.partial(act, stage + str(i)) for i in range(4) if PLAN.get(stage + str(i))}

    def up_rows(i, left, pre, post):
        for n in range(0, pre.shape[1], LANES):
            z = mat_nn(left, wu[:, n:n + LANES]).astype(bf16)
            pre[tile_rows(i), n:n + LANES] = z
            post[tile_rows(i), n:n + LANES] = gelu(z.astype(f32)).astype(bf16)

    def cot_rows(i, cot, pre):
        for n in range(0, pre.shape[1], LANES):
            c = mat_nt(cot, wd[n:n + LANES, :])
            z = pre[tile_rows(i), n:n + LANES].astype(f32)
            pre[tile_rows(i), n:n + LANES] = (gelu_slope(z) * c).astype(bf16)

    def put_trans(i, value):
        trans[:, tile_rows(i)] = value.T.astype(bf16)

    def full_product(acc, right, key=None):
        for n in range(0, acc.shape[1], 256):
            if key and n == acc.shape[1] // 2:
                act(key)
            acc[:, n:n + 256] = mat_nn(trans[...], right[:, n:n + 256])

    def add_product(i, acc, left, right):
        @pl.when(i == 0)
        def _():
            acc[...] = jnp.zeros_like(acc)
        for n in range(0, acc.shape[1], 256):
            acc[:, n:n + 256] += mat_nn(left, right[:, n:n + 256])

    def normalise(acc, out, row, index, dst):
        def run(k, carry):
            rows = pl.ds(pl.multiple_of(k * 32, 32), 32)
            p = acc[rows, :]
            out[pl.ds(pl.multiple_of(row + k * 32, 32), 32), :] = (p / jnp.sqrt(jnp.sum(p * p, axis=1, keepdims=True))).astype(bf16)
            return carry
        lax.fori_loop(0, 8, run, 0)
        pltpu.make_async_copy(out.at[row:row + 256], dst, out_sem.at[index]).start()

    def z0_stage(i, x_tile):
        up_rows(i, x_tile[...], z0, a0)

    load_wu0.wait()
    streamed(x_hbm, x_hbm, z0_stage)
    load_wu1.start()
    load_wd0.wait()

    def h1_stage(i, x_tile):
        for n in range(0, h1.shape[1], 256):
            h1[tile_rows(i), n:n + 256] = (x_tile[:, n:n + 256].astype(f32) + mat_nn(a0[tile_rows(i), :], wd[:, n:n + 256])).astype(bf16)
    streamed(x_hbm, dy_hbm, h1_stage)
    load_wd1.start()
    load_wu1.wait()
    loop(lambda i: up_rows(i, h1[tile_rows(i), :], z1, a1))
    load_qd1.wait()

    def sd1_stage(i, dy_tile):
        put_trans(i, mat_nn(dy_tile[...], qd[...]))
    streamed(dy_hbm, dy_hbm, sd1_stage)
    load_qd0.start()
    full_product(pd1, a1)
    advance("d1")
    load_wd1.wait()
    load_qu1.wait()

    def e1_stage(i, dy_tile):
        cot_rows(i, dy_tile[...], z1)
        put_trans(i, mat_nn(z1[tile_rows(i), :], qu[...]))
    streamed(dy_hbm, dy_hbm, e1_stage, hooks("e1_"))
    load_wd0b.start()
    load_qu0.start()
    act("pu1")
    full_product(pu1, h1)
    advance("u1")

    def g1_stage(i, dy_tile):
        for n in range(0, g1.shape[1], 256):
            g1[tile_rows(i), n:n + 256] = (dy_tile[:, n:n + 256].astype(f32) + mat_nt(z1[tile_rows(i), :], wu[n:n + 256, :])).astype(bf16)
    streamed(dy_hbm, x_hbm, g1_stage, hooks("g1_"))
    load_qd0.wait()
    loop(lambda i: put_trans(i, mat_nn(g1[tile_rows(i), :], qd[...])), hooks("sd0_"))
    act("pd0")
    full_product(pd0, a0, "pd0m")
    advance("d0")
    load_wd0b.wait()
    load_qu0.wait()

    def e0_stage(i, x_tile):
        cot_rows(i, g1[tile_rows(i), :], z0)
        sketch = mat_nn(z0[tile_rows(i), :], qu[...]).T.astype(bf16)
        add_product(i, pu0, sketch, x_tile)
    streamed(x_hbm, dy_hbm, e0_stage, hooks("e0_"))
    advance("u0")
    act("hats1")
    normalise(pu1, wd, 0, 1, hat_u_hbm.at[1])

    def qd1_stage(i, dy_tile):
        back = mat_nt(a1[tile_rows(i), :], wu[0:256, :]).T.astype(bf16)
        add_product(i, pu1, back, dy_tile)
    streamed(dy_hbm, x_hbm, qd1_stage, hooks("qd1_"))
    advance("qd1")
    loop(lambda i: put_trans(i, mat_nt(h1[tile_rows(i), :], wd[0:256, :])), hooks("uu1_"))
    act("qu1")
    full_product(pd1, z1, "qu1m")
    advance("qu1")
    act("hd0")
    normalise(pd0, wu, 256, 2, hat_d_hbm.at[0])
    act("hu0")
    normalise(pu0, wd, 256, 3, hat_u_hbm.at[0])

    def uu0_stage(i, x_tile):
        put_trans(i, mat_nt(x_tile[...], wd[256:512, :]))
    streamed(x_hbm, None, uu0_stage, hooks("uu0_"))
    act("qu0")
    full_product(pd0, z0, "qu0m")
    advance("qu0")
    loop(lambda i: put_trans(i, mat_nt(a0[tile_rows(i), :], wu[256:512, :])), hooks("ud0_"))
    act("qd0")
    full_product(pu0, g1)
    advance("qd0")
    act("end")
    assert set(phases.values()) == {8}
    hats = [(wu, 0, hat_d_hbm.at[1]), (wd, 0, hat_u_hbm.at[1]), (wu, 256, hat_d_hbm.at[0]), (wd, 256, hat_u_hbm.at[0])]
    for k, (src, row, dst) in enumerate(hats):
        pltpu.make_async_copy(src.at[row:row + 256], dst, out_sem.at[k]).wait()
    for copy in outs.values():
        copy.wait()


def sum_scratch(lanes):
    return [pltpu.VMEM((128, lanes), jnp.float32), pltpu.VMEM((3, 32, lanes), jnp.float32), pltpu.VMEM((3, 8, lanes), jnp.float32), pltpu.VMEM((3, 8, lanes), jnp.float32), pltpu.SemaphoreType.DMA((COPIES,)), pltpu.SemaphoreType.DMA((COPIES,)), pltpu.SemaphoreType.REGULAR]


def power_sums(axis, tok_rows, grad_rows, w_up, w_down, q_up, q_down):
    tokens, model = tok_rows.shape
    layers, _, wide = w_up.shape
    rank = q_up.shape[-1]
    bf16, f32 = jnp.bfloat16, jnp.float32
    scratch = [pltpu.VMEM((tokens, wide), bf16)] * 4 + [pltpu.VMEM((tokens, model), bf16)] * 2
    scratch += [pltpu.VMEM((model, wide), bf16), pltpu.VMEM((wide, model), bf16), pltpu.VMEM((wide, rank), bf16), pltpu.VMEM((model, rank), bf16)]
    scratch += [pltpu.VMEM((rank, tokens), bf16), pltpu.VMEM((2, TILE, model), bf16)]
    scratch += [pltpu.VMEM((rank, lanes), f32) for lanes in (wide, model, wide, model)]
    scratch += [pltpu.SemaphoreType.DMA((2,)), pltpu.SemaphoreType.DMA((9,)), pltpu.SemaphoreType.DMA((8,))]
    for lanes in (wide, wide, model, model):
        scratch += sum_scratch(lanes)
    return pl.pallas_call(
        functools.partial(step_kernel, axis),
        out_shape=[jax.ShapeDtypeStruct((layers, rank, model), bf16), jax.ShapeDtypeStruct((layers, rank, wide), bf16), jax.ShapeDtypeStruct((layers, rank, wide), f32), jax.ShapeDtypeStruct((layers, rank, model), f32)],
        in_specs=[pl.BlockSpec(memory_space=pl.ANY)] * 6,
        out_specs=[pl.BlockSpec(memory_space=pl.ANY)] * 4,
        scratch_shapes=scratch,
        compiler_params=pltpu.CompilerParams(collective_id=0, has_side_effects=True, vmem_limit_bytes=67043328),
        name="power_sums",
    )(tok_rows, grad_rows, w_up, w_down, q_up, q_down)


def update_kernel(step_size, hat_u_hbm, hat_d_hbm, sum_u_hbm, sum_d_hbm, wu_hbm, wd_hbm, wu_out, wd_out, fac_u_out, fac_d_out,
                  hat_u, hat_d, sum_u, sum_d, wu, wd, turn_u, turn_d, small_sem, w_sem, out_sem, fac_sem):
    layers, model, wide = wu.shape
    rank = hat_u.shape[1]
    bf16, f32 = jnp.bfloat16, jnp.float32
    order = tuple(reversed(range(layers)))
    chunk_u, chunk_d = model // 3, wide // 4

    def small(l, k, src, dst):
        return pltpu.make_async_copy(src.at[l], dst.at[l], small_sem.at[l, k])

    def part(l, k):
        if k < 3:
            return wu_hbm.at[l, k * chunk_u:(k + 1) * chunk_u], wu.at[l, k * chunk_u:(k + 1) * chunk_u], wu_out.at[l, k * chunk_u:(k + 1) * chunk_u]
        rows = slice((k - 3) * chunk_d, (k - 2) * chunk_d)
        return wd_hbm.at[l, rows], wd.at[l, rows], wd_out.at[l, rows]

    smalls = {}
    loads = {}
    for l in order:
        smalls[l] = [small(l, 0, sum_u_hbm, sum_u), small(l, 1, hat_u_hbm, hat_u), small(l, 2, sum_d_hbm, sum_d), small(l, 3, hat_d_hbm, hat_d)]
        for k in range(7):
            src, dst, _ = part(l, k)
            loads[l, k] = pltpu.make_async_copy(src, dst, w_sem.at[l, k])
        for copy in smalls[l][:2] + [loads[l, k] for k in range(3)] + smalls[l][2:] + [loads[l, k] for k in range(3, 7)]:
            copy.start()
    stores = []

    def store(src, dst, sem):
        copy = pltpu.make_async_copy(src, dst, sem)
        copy.start()
        stores.append(copy)

    for l in order:
        for k in range(7):
            total, hat, w, turn, out, first = (sum_u, hat_u, wu, turn_u, fac_u_out, 0) if k < 3 else (sum_d, hat_d, wd, turn_d, fac_d_out, 3)
            width, count = (chunk_u, 3) if k < 3 else (chunk_d, 4)
            row = (k - first) * width
            if k == first:
                smalls[l][0 if k < 3 else 2].wait()
                smalls[l][1 if k < 3 else 3].wait()
            span = total.shape[2] // (4 if k < 3 else 3)
            for j in range(span and (4 if k < 3 else 3)):
                if k == first:
                    turn[l, j * span:(j + 1) * span, :] = total[l, :, j * span:(j + 1) * span].T
            if k == first:
                store(turn.at[l], out.at[l], fac_sem.at[l, 0 if k < 3 else 1])
            loads[l, k].wait()
            left = hat[l, :, row:row + width]
            lanes = 512 if k < 3 else 384
            for n in range(0, w.shape[2], lanes):
                step = step_size * mat_tn(left, total[l, :, n:n + lanes].astype(bf16))
                w[l, row:row + width, n:n + lanes] = (w[l, row:row + width, n:n + lanes].astype(f32) - step).astype(bf16)
            _, src, dst = part(l, k)
            store(src, dst, out_sem.at[l, k])
    for copy in stores:
        copy.wait()


def update(step_size, hat_u, hat_d, sum_u, sum_d, w_up, w_down):
    layers, model, wide = w_up.shape
    rank = hat_u.shape[1]
    bf16, f32 = jnp.bfloat16, jnp.float32
    return pl.pallas_call(
        functools.partial(update_kernel, step_size),
        in_specs=[pl.BlockSpec(memory_space=pl.ANY)] * 6,
        out_specs=[pl.BlockSpec(memory_space=pl.ANY)] * 4,
        out_shape=[jax.ShapeDtypeStruct((layers, model, wide), bf16), jax.ShapeDtypeStruct((layers, wide, model), bf16), jax.ShapeDtypeStruct((layers, wide, rank), f32), jax.ShapeDtypeStruct((layers, model, rank), f32)],
        scratch_shapes=[pltpu.VMEM(hat_u.shape, bf16), pltpu.VMEM(hat_d.shape, bf16), pltpu.VMEM(sum_u.shape, f32), pltpu.VMEM(sum_d.shape, f32), pltpu.VMEM(w_up.shape, bf16), pltpu.VMEM(w_down.shape, bf16), pltpu.VMEM((layers, wide, rank), f32), pltpu.VMEM((layers, model, rank), f32), pltpu.SemaphoreType.DMA((layers, 4)), pltpu.SemaphoreType.DMA((layers, 7)), pltpu.SemaphoreType.DMA((layers, 7)), pltpu.SemaphoreType.DMA((layers, 2))],
        compiler_params=pltpu.CompilerParams(vmem_limit_bytes=60 * 2**20),
        name="update",
    )(hat_u, hat_d, sum_u, sum_d, w_up, w_down)


def solution(mesh):
    axis = mesh.axis_names[0]

    def local_step(tok_rows, grad_rows, w_up, w_down, q_up, q_down):
        step_size = 0.4 / math.sqrt(q_up.shape[-1])
        hat_u, hat_d, sum_u, sum_d = power_sums(axis, tok_rows, grad_rows, w_up, w_down, q_up, q_down)
        return tuple(update(step_size, hat_u, hat_d, sum_u, sum_d, w_up, w_down))

    row_spec = P(axis, None)
    return jax.shard_map(local_step, mesh=mesh, in_specs=(row_spec, row_spec, P(), P(), P(), P()), out_specs=(P(), P(), P(), P()), check_vma=False)
```

```python
import math
import functools
import jax
import jax.numpy as jnp
from jax import lax
from jax.experimental import pallas as pl
from jax.experimental.pallas import tpu as pltpu
from jax.sharding import PartitionSpec as P

MESH = pl.DeviceIdType.MESH
STRIDES = (2, 8, 32)
ORDERS = ((0, 1, 2), (1, 2, 0), (2, 0, 1))
COPIES = 47


def mat_nn(left_op, right_op):
    return jnp.dot(left_op, right_op, preferred_element_type=jnp.float32)


def mat_nt(left_op, right_op):
    return lax.dot_general(left_op, right_op, (((1,), (1,)), ((), ())), preferred_element_type=jnp.float32)


def mat_tn(left_op, right_op):
    return lax.dot_general(left_op, right_op, (((0,), (0,)), ((), ())), preferred_element_type=jnp.float32)


def flip(place, bit):
    if bit == 1:
        return place + 1 - 2 * lax.rem(place, 2)
    if bit == 2:
        return lax.rem(place + 2, 4)
    return 3 - place


def position(axis):
    me = lax.axis_index(axis)
    core = lax.rem(me, 2)
    places = tuple(lax.rem(lax.div(me, stride), 4) for stride in STRIDES)
    return me, core, places


def greet(pos):
    me, core, places = pos
    barrier = pltpu.get_barrier_semaphore()
    pl.semaphore_signal(barrier, inc=1, device_id=(me + 1 - 2 * core,), device_id_type=MESH)
    for dim in range(3):
        for bit in (1, 2, 3):
            peer = me + (flip(places[dim], bit) - places[dim]) * STRIDES[dim]
            pl.semaphore_signal(barrier, inc=1, device_id=(peer,), device_id_type=MESH)
    pl.semaphore_wait(barrier, 10)


class SumAll:
    def __init__(self, acc, bufs, sems, pos, lanes):
        self.acc, self.bufs, self.sems, self.pos = acc, bufs, sems, pos
        third = lanes // 3 // 128 * 128
        self.groups = ((0, third), (third, third), (2 * third, lanes - 2 * third))

    def rows(self, start, size, lo, width):
        return self.acc.at[pl.ds(pl.multiple_of(start, 8), size), pl.ds(lo, width)]

    def copies(self, phase):
        me, core, places = self.pos
        send, recv = self.sems[:2]
        lanes = self.acc.shape[1]
        out = []

        def add(index, src, dst, peer):
            out.append(pltpu.make_async_remote_copy(src_ref=src, dst_ref=dst, send_sem=send.at[index], recv_sem=recv.at[index], device_id=(peer,), device_id_type=MESH))

        partner = me + 1 - 2 * core
        if phase == 0:
            add(0, self.rows((1 - core) * 128, 128, 0, lanes), self.bufs[0], partner)
            return out
        if phase == 6:
            mine = self.rows(core * 128, 128, 0, lanes)
            add(46, mine, mine, partner)
            return out
        for group, (lo, width) in enumerate(self.groups):
            first, second, third = ORDERS[group]
            top = core * 128
            block = top + places[first] * 32
            base = block + places[second] * 8
            dim = {1: first, 2: second, 3: third, 4: second, 5: first}[phase]
            for bit in (1, 2, 3):
                other = flip(places[dim], bit)
                peer = me + (other - places[dim]) * STRIDES[dim]
                index = 1 + (phase - 1) * 9 + group * 3 + bit - 1
                if phase == 1:
                    src, dst = self.rows(top + other * 32, 32, lo, width), self.bufs[1].at[bit - 1, :, pl.ds(lo, width)]
                elif phase == 2:
                    src, dst = self.rows(block + other * 8, 8, lo, width), self.bufs[2].at[bit - 1, :, pl.ds(lo, width)]
                elif phase == 3:
                    src, dst = self.rows(base, 8, lo, width), self.bufs[3].at[bit - 1, :, pl.ds(lo, width)]
                elif phase == 4:
                    src = dst = self.rows(base, 8, lo, width)
                else:
                    src = dst = self.rows(block, 32, lo, width)
                add(index, src, dst, peer)
        return out

    def start(self, phase):
        if phase == 6:
            pl.semaphore_wait(self.sems[2], 1)
        for copy in self.copies(phase):
            copy.start()

    def finish(self, phase):
        for copy in self.copies(phase):
            copy.wait()
        me, core, places = self.pos
        if phase == 0:
            pl.semaphore_signal(self.sems[2], inc=1, device_id=(me + 1 - 2 * core,), device_id_type=MESH)
            def add(k, carry):
                mine = self.rows(core * 128 + k * 8, 8, 0, self.acc.shape[1])
                mine[...] += self.bufs[0][pl.ds(pl.multiple_of(k * 8, 8), 8), :]
                return carry
            lax.fori_loop(0, 16, add, 0)
            return
        if phase > 3:
            return
        for group, (lo, width) in enumerate(self.groups):
            first, second, third = ORDERS[group]
            block = core * 128 + places[first] * 32
            for k in range(4 if phase == 1 else 1):
                got = [self.bufs[phase][bit, k * 8:k * 8 + 8, pl.ds(lo, width)] for bit in range(3)]
                mine = self.rows(block + k * 8 if phase == 1 else block + places[second] * 8, 8, lo, width)
                mine[...] = (mine[...] + got[0]) + (got[1] + got[2])

    def step(self, phase):
        if phase > 0:
            self.finish(phase - 1)
        if phase < 7:
            self.start(phase)


PLAN = {'e1_1': ('d1',),
 'pu1': ('d1',),
 'g1_2': ('u1', 'd1'),
 'sd0_1': ('d1', 'u1'),
 'e0_1': ('d1', 'u1', 'd0'),
 'e0_3': ('d1', 'u1'),
 'hats1': ('d0', 'd1', 'u1', 'u0', 'u1', 'd0', 'u1', 'u0', 'd0', 'hd1'),
 'qd1_1': ('u0',),
 'qd1_2': ('d0',),
 'qd1_3': ('u0',),
 'qu1': ('qd1', 'd0'),
 'qu1m': ('u0',),
 'hd0': ('d0',),
 'hu0': ('u0', 'qd1', 'qu1', 'u0'),
 'uu0_2': ('qd1',),
 'ud0_0': ('qd1', 'qu1'),
 'qd0': ('qu0',),
 'end': ('qd1',
         'qu1',
         'qd0',
         'qd1',
         'qu0',
         'qu1',
         'qd1',
         'qd0',
         'qu0',
         'qu1',
         'qd0',
         'qu0',
         'qu1',
         'qd0',
         'qu0',
         'qu1',
         'qd0',
         'qu0',
         'qd0',
         'qu0',
         'qd0')}
TILE = 512
LANES = 256
ROOT = math.sqrt(2.0 / math.pi)


def gelu(z):
    half = 0.5 * z
    return half + half * jnp.tanh(z * (ROOT + (ROOT * 0.044715) * (z * z)))


def gelu_slope(z):
    square = z * z
    t = jnp.tanh(z * (ROOT + (ROOT * 0.044715) * square))
    more = 1.0 + t
    return 0.5 * more + (more * z) * ((1.0 - t) * (0.5 * ROOT + (1.5 * ROOT * 0.044715) * square))


def tile_rows(i):
    return pl.ds(pl.multiple_of(i * TILE, TILE), TILE)


def step_kernel(axis, *refs):
    (x_hbm, dy_hbm, wu_hbm, wd_hbm, qu_hbm, qd_hbm, hat_u_hbm, hat_d_hbm, sum_u_hbm, sum_d_hbm,
     a0, z0, a1, z1, h1, g1, wu, wd, qu, qd, trans, stream_buf, pd1, pu1, pd0, pu0,
     stream_sem, load_sem, out_sem, *rest) = refs
    tiles = x_hbm.shape[0] // TILE
    bf16 = jnp.bfloat16
    f32 = jnp.float32
    channels = [rest[7 * k:7 * k + 7] for k in range(4)]

    def load(index, src, dst):
        return pltpu.make_async_copy(src, dst, load_sem.at[index])

    def tile_copy(src, i, slot):
        return pltpu.make_async_copy(src.at[tile_rows(i)], stream_buf.at[slot], stream_sem.at[slot])

    def loop(body, hooks=None):
        def run(i, carry):
            for when, hook in (hooks or {}).items():
                pl.when(i == when)(hook)
            body(i)
            return carry
        lax.fori_loop(0, tiles, run, 0)

    def streamed(src, following, body, hooks=None):
        def run(i):
            slot = lax.rem(i, 2)

            @pl.when(i + 1 < tiles)
            def _():
                tile_copy(src, i + 1, 1 - slot).start()
            tile_copy(src, i, slot).wait()
            body(i, stream_buf.at[slot])
        loop(run, hooks)
        if following is not None:
            tile_copy(following, 0, 0).start()

    tile_copy(x_hbm, 0, 0).start()
    load_wu0 = load(0, wu_hbm.at[0], wu)
    load_wd0 = load(1, wd_hbm.at[0], wd)
    load_qd1 = load(2, qd_hbm.at[1], qd)
    load_qu1 = load(3, qu_hbm.at[1], qu)
    load_wu1 = load(4, wu_hbm.at[1], wu)
    load_wd1 = load(5, wd_hbm.at[1], wd)
    load_wd0b = load(6, wd_hbm.at[0], wd)
    load_qd0 = load(7, qd_hbm.at[0], qd)
    load_qu0 = load(8, qu_hbm.at[0], qu)
    load_wu0.start()
    load_wd0.start()
    load_qd1.start()
    load_qu1.start()
    pos = position(axis)
    greet(pos)

    def reducer(acc, channel):
        return SumAll(acc, channels[channel][:4], channels[channel][4:], pos, acc.shape[1])

    places = {"d1": (pd1, 0), "u1": (pu1, 2), "d0": (pd0, 1), "u0": (pu0, 3), "qd1": (pu1, 2), "qu1": (pd1, 0), "qd0": (pu0, 3), "qu0": (pd0, 1)}
    sums = {name: reducer(*place) for name, place in places.items()}
    phases = dict.fromkeys(places, 0)
    spots = {"qd1": sum_d_hbm.at[1], "qu1": sum_u_hbm.at[1], "qd0": sum_d_hbm.at[0], "qu0": sum_u_hbm.at[0]}
    outs = {name: pltpu.make_async_copy(places[name][0], spot, out_sem.at[4 + k]) for k, (name, spot) in enumerate(spots.items())}

    def act(key):
        for name in PLAN.get(key, ()):
            if name == "hd1":
                normalise(pd1, wu, 0, 0, hat_d_hbm.at[1])
            else:
                advance(name)

    def advance(name):
        sums[name].step(phases[name])
        phases[name] += 1
        if phases[name] == 8 and name in outs:
            outs[name].start()

    def hooks(stage):
        return {i: functools.partial(act, stage + str(i)) for i in range(4) if PLAN.get(stage + str(i))}

    def up_rows(i, left, pre, post):
        for n in range(0, pre.shape[1], LANES):
            z = mat_nn(left, wu[:, n:n + LANES]).astype(bf16)
            pre[tile_rows(i), n:n + LANES] = z
            post[tile_rows(i), n:n + LANES] = gelu(z.astype(f32)).astype(bf16)

    def cot_rows(i, cot, pre):
        for n in range(0, pre.shape[1], LANES):
            c = mat_nt(cot, wd[n:n + LANES, :])
            z = pre[tile_rows(i), n:n + LANES].astype(f32)
            pre[tile_rows(i), n:n + LANES] = (gelu_slope(z) * c).astype(bf16)

    def put_trans(i, value):
        trans[:, tile_rows(i)] = value.T.astype(bf16)

    def full_product(acc, right, key=None):
        for n in range(0, acc.shape[1], 256):
            if key and n == acc.shape[1] // 2:
                act(key)
            acc[:, n:n + 256] = mat_nn(trans[...], right[:, n:n + 256])

    def add_product(i, acc, left, right):
        @pl.when(i == 0)
        def _():
            acc[...] = jnp.zeros_like(acc)
        for n in range(0, acc.shape[1], 256):
            acc[:, n:n + 256] += mat_nn(left, right[:, n:n + 256])

    def normalise(acc, out, row, index, dst):
        def run(k, carry):
            rows = pl.ds(pl.multiple_of(k * 32, 32), 32)
            p = acc[rows, :]
            out[pl.ds(pl.multiple_of(row + k * 32, 32), 32), :] = (p / jnp.sqrt(jnp.sum(p * p, axis=1, keepdims=True))).astype(bf16)
            return carry
        lax.fori_loop(0, 8, run, 0)
        pltpu.make_async_copy(out.at[row:row + 256], dst, out_sem.at[index]).start()

    def z0_stage(i, x_tile):
        up_rows(i, x_tile[...], z0, a0)

    load_wu0.wait()
    streamed(x_hbm, x_hbm, z0_stage)
    load_wu1.start()
    load_wd0.wait()

    def h1_stage(i, x_tile):
        for n in range(0, h1.shape[1], 256):
            h1[tile_rows(i), n:n + 256] = (x_tile[:, n:n + 256].astype(f32) + mat_nn(a0[tile_rows(i), :], wd[:, n:n + 256])).astype(bf16)
    streamed(x_hbm, dy_hbm, h1_stage)
    load_wd1.start()
    load_wu1.wait()
    loop(lambda i: up_rows(i, h1[tile_rows(i), :], z1, a1))
    load_qd1.wait()

    def sd1_stage(i, dy_tile):
        put_trans(i, mat_nn(dy_tile[...], qd[...]))
    streamed(dy_hbm, dy_hbm, sd1_stage)
    load_qd0.start()
    full_product(pd1, a1)
    advance("d1")
    load_wd1.wait()
    load_qu1.wait()

    def e1_stage(i, dy_tile):
        cot_rows(i, dy_tile[...], z1)
        put_trans(i, mat_nn(z1[tile_rows(i), :], qu[...]))
    streamed(dy_hbm, dy_hbm, e1_stage, hooks("e1_"))
    load_wd0b.start()
    load_qu0.start()
    act("pu1")
    full_product(pu1, h1)
    advance("u1")

    def g1_stage(i, dy_tile):
        for n in range(0, g1.shape[1], 256):
            g1[tile_rows(i), n:n + 256] = (dy_tile[:, n:n + 256].astype(f32) + mat_nt(z1[tile_rows(i), :], wu[n:n + 256, :])).astype(bf16)
    streamed(dy_hbm, x_hbm, g1_stage, hooks("g1_"))
    load_qd0.wait()
    loop(lambda i: put_trans(i, mat_nn(g1[tile_rows(i), :], qd[...])), hooks("sd0_"))
    act("pd0")
    full_product(pd0, a0, "pd0m")
    advance("d0")
    load_wd0b.wait()
    load_qu0.wait()

    def e0_stage(i, x_tile):
        cot_rows(i, g1[tile_rows(i), :], z0)
        sketch = mat_nn(z0[tile_rows(i), :], qu[...]).T.astype(bf16)
        add_product(i, pu0, sketch, x_tile)
    streamed(x_hbm, dy_hbm, e0_stage, hooks("e0_"))
    advance("u0")
    act("hats1")
    normalise(pu1, wd, 0, 1, hat_u_hbm.at[1])

    def qd1_stage(i, dy_tile):
        back = mat_nt(a1[tile_rows(i), :], wu[0:256, :]).T.astype(bf16)
        add_product(i, pu1, back, dy_tile)
    streamed(dy_hbm, x_hbm, qd1_stage, hooks("qd1_"))
    advance("qd1")
    loop(lambda i: put_trans(i, mat_nt(h1[tile_rows(i), :], wd[0:256, :])), hooks("uu1_"))
    act("qu1")
    full_product(pd1, z1, "qu1m")
    advance("qu1")
    act("hd0")
    normalise(pd0, wu, 256, 2, hat_d_hbm.at[0])
    act("hu0")
    normalise(pu0, wd, 256, 3, hat_u_hbm.at[0])

    def uu0_stage(i, x_tile):
        put_trans(i, mat_nt(x_tile[...], wd[256:512, :]))
    streamed(x_hbm, None, uu0_stage, hooks("uu0_"))
    act("qu0")
    full_product(pd0, z0, "qu0m")
    advance("qu0")
    loop(lambda i: put_trans(i, mat_nt(a0[tile_rows(i), :], wu[256:512, :])), hooks("ud0_"))
    act("qd0")
    full_product(pu0, g1)
    advance("qd0")
    act("end")
    assert set(phases.values()) == {8}
    hats = [(wu, 0, hat_d_hbm.at[1]), (wd, 0, hat_u_hbm.at[1]), (wu, 256, hat_d_hbm.at[0]), (wd, 256, hat_u_hbm.at[0])]
    for k, (src, row, dst) in enumerate(hats):
        pltpu.make_async_copy(src.at[row:row + 256], dst, out_sem.at[k]).wait()
    for copy in outs.values():
        copy.wait()


def sum_scratch(lanes):
    return [pltpu.VMEM((128, lanes), jnp.float32), pltpu.VMEM((3, 32, lanes), jnp.float32), pltpu.VMEM((3, 8, lanes), jnp.float32), pltpu.VMEM((3, 8, lanes), jnp.float32), pltpu.SemaphoreType.DMA((COPIES,)), pltpu.SemaphoreType.DMA((COPIES,)), pltpu.SemaphoreType.REGULAR]


def power_sums(axis, tok_rows, grad_rows, w_up, w_down, q_up, q_down):
    tokens, model = tok_rows.shape
    layers, _, wide = w_up.shape
    rank = q_up.shape[-1]
    bf16, f32 = jnp.bfloat16, jnp.float32
    scratch = [pltpu.VMEM((tokens, wide), bf16)] * 4 + [pltpu.VMEM((tokens, model), bf16)] * 2
    scratch += [pltpu.VMEM((model, wide), bf16), pltpu.VMEM((wide, model), bf16), pltpu.VMEM((wide, rank), bf16), pltpu.VMEM((model, rank), bf16)]
    scratch += [pltpu.VMEM((rank, tokens), bf16), pltpu.VMEM((2, TILE, model), bf16)]
    scratch += [pltpu.VMEM((rank, lanes), f32) for lanes in (wide, model, wide, model)]
    scratch += [pltpu.SemaphoreType.DMA((2,)), pltpu.SemaphoreType.DMA((9,)), pltpu.SemaphoreType.DMA((8,))]
    for lanes in (wide, wide, model, model):
        scratch += sum_scratch(lanes)
    return pl.pallas_call(
        functools.partial(step_kernel, axis),
        out_shape=[jax.ShapeDtypeStruct((layers, rank, model), bf16), jax.ShapeDtypeStruct((layers, rank, wide), bf16), jax.ShapeDtypeStruct((layers, rank, wide), f32), jax.ShapeDtypeStruct((layers, rank, model), f32)],
        in_specs=[pl.BlockSpec(memory_space=pl.ANY)] * 6,
        out_specs=[pl.BlockSpec(memory_space=pl.ANY)] * 4,
        scratch_shapes=scratch,
        compiler_params=pltpu.CompilerParams(collective_id=0, has_side_effects=True, vmem_limit_bytes=67043328),
        name="power_sums",
    )(tok_rows, grad_rows, w_up, w_down, q_up, q_down)


def update_kernel(step_size, hat_u_hbm, hat_d_hbm, sum_u_hbm, sum_d_hbm, wu_hbm, wd_hbm, wu_out, wd_out, fac_u_out, fac_d_out,
                  hat_u, hat_d, sum_u, sum_d, wu, wd, turn_u, turn_d, small_sem, w_sem, out_sem, fac_sem):
    layers, model, wide = wu.shape
    rank = hat_u.shape[1]
    bf16, f32 = jnp.bfloat16, jnp.float32
    order = tuple(reversed(range(layers)))
    chunk_u, chunk_d = model // 3, wide // 4

    def small(l, k, src, dst):
        return pltpu.make_async_copy(src.at[l], dst.at[l], small_sem.at[l, k])

    def part(l, k):
        if k < 3:
            return wu_hbm.at[l, k * chunk_u:(k + 1) * chunk_u], wu.at[l, k * chunk_u:(k + 1) * chunk_u], wu_out.at[l, k * chunk_u:(k + 1) * chunk_u]
        rows = slice((k - 3) * chunk_d, (k - 2) * chunk_d)
        return wd_hbm.at[l, rows], wd.at[l, rows], wd_out.at[l, rows]

    def smalls(l, half):
        pairs = ((sum_d_hbm, sum_d), (hat_d_hbm, hat_d)) if half else ((sum_u_hbm, sum_u), (hat_u_hbm, hat_u))
        return [small(l, 2 * half + k, src, dst) for k, (src, dst) in enumerate(pairs)]

    def load(l, k):
        src, dst, _ = part(l, k)
        return pltpu.make_async_copy(src, dst, w_sem.at[l, k])

    def store(l, k):
        _, src, dst = part(l, k)
        return pltpu.make_async_copy(src, dst, out_sem.at[l, k])

    def store_fac(l, half):
        return pltpu.make_async_copy((turn_d if half else turn_u).at[l], (fac_d_out if half else fac_u_out).at[l], fac_sem.at[l, half])

    for l in order:
        for copy in smalls(l, 0) + [load(l, k) for k in range(3)] + smalls(l, 1) + [load(l, k) for k in range(3, 7)]:
            copy.start()

    def run(index, carry):
        l = layers - 1 - index
        for half, (total, hat, w, turn, width, count, lanes) in enumerate(((sum_u, hat_u, wu, turn_u, chunk_u, 3, 512), (sum_d, hat_d, wd, turn_d, chunk_d, 4, 384))):
            for copy in smalls(l, half):
                copy.wait()
            for n in range(0, total.shape[2], lanes):
                turn[l, n:n + lanes, :] = total[l, :, n:n + lanes].T
            store_fac(l, half).start()
            for k in range(count):
                load(l, 3 * half + k).wait()
                rows = slice(k * width, (k + 1) * width)
                for n in range(0, w.shape[2], lanes):
                    step = step_size * mat_tn(hat[l, :, rows], total[l, :, n:n + lanes].astype(bf16))
                    w[l, rows, n:n + lanes] = (w[l, rows, n:n + lanes].astype(f32) - step).astype(bf16)
                store(l, 3 * half + k).start()
        return carry

    lax.fori_loop(0, layers, run, 0)
    for l in order:
        for k in range(7):
            store(l, k).wait()
        for half in range(2):
            store_fac(l, half).wait()


def update(step_size, hat_u, hat_d, sum_u, sum_d, w_up, w_down):
    layers, model, wide = w_up.shape
    rank = hat_u.shape[1]
    bf16, f32 = jnp.bfloat16, jnp.float32
    return pl.pallas_call(
        functools.partial(update_kernel, step_size),
        in_specs=[pl.BlockSpec(memory_space=pl.ANY)] * 6,
        out_specs=[pl.BlockSpec(memory_space=pl.ANY)] * 4,
        out_shape=[jax.ShapeDtypeStruct((layers, model, wide), bf16), jax.ShapeDtypeStruct((layers, wide, model), bf16), jax.ShapeDtypeStruct((layers, wide, rank), f32), jax.ShapeDtypeStruct((layers, model, rank), f32)],
        scratch_shapes=[pltpu.VMEM(hat_u.shape, bf16), pltpu.VMEM(hat_d.shape, bf16), pltpu.VMEM(sum_u.shape, f32), pltpu.VMEM(sum_d.shape, f32), pltpu.VMEM(w_up.shape, bf16), pltpu.VMEM(w_down.shape, bf16), pltpu.VMEM((layers, wide, rank), f32), pltpu.VMEM((layers, model, rank), f32), pltpu.SemaphoreType.DMA((layers, 4)), pltpu.SemaphoreType.DMA((layers, 7)), pltpu.SemaphoreType.DMA((layers, 7)), pltpu.SemaphoreType.DMA((layers, 2))],
        compiler_params=pltpu.CompilerParams(vmem_limit_bytes=60 * 2**20),
        name="update",
    )(hat_u, hat_d, sum_u, sum_d, w_up, w_down)


def solution(mesh):
    axis = mesh.axis_names[0]

    def local_step(tok_rows, grad_rows, w_up, w_down, q_up, q_down):
        step_size = 0.4 / math.sqrt(q_up.shape[-1])
        hat_u, hat_d, sum_u, sum_d = power_sums(axis, tok_rows, grad_rows, w_up, w_down, q_up, q_down)
        return tuple(update(step_size, hat_u, hat_d, sum_u, sum_d, w_up, w_down))

    row_spec = P(axis, None)
    return jax.shard_map(local_step, mesh=mesh, in_specs=(row_spec, row_spec, P(), P(), P(), P()), out_specs=(P(), P(), P(), P()), check_vma=False)
```

```python
import math
import functools
import jax
import jax.numpy as jnp
from jax import lax
from jax.experimental import pallas as pl
from jax.experimental.pallas import tpu as pltpu
from jax.sharding import PartitionSpec as P

MESH = pl.DeviceIdType.MESH
STRIDES = (2, 8, 32)
ORDERS = ((0, 1, 2), (1, 2, 0), (2, 0, 1))
COPIES = 47


def mat_nn(left_op, right_op):
    return jnp.dot(left_op, right_op, preferred_element_type=jnp.float32)


def mat_nt(left_op, right_op):
    return lax.dot_general(left_op, right_op, (((1,), (1,)), ((), ())), preferred_element_type=jnp.float32)


def mat_tn(left_op, right_op):
    return lax.dot_general(left_op, right_op, (((0,), (0,)), ((), ())), preferred_element_type=jnp.float32)


def flip(place, bit):
    if bit == 1:
        return place + 1 - 2 * lax.rem(place, 2)
    if bit == 2:
        return lax.rem(place + 2, 4)
    return 3 - place


def position(axis):
    me = lax.axis_index(axis)
    core = lax.rem(me, 2)
    places = tuple(lax.rem(lax.div(me, stride), 4) for stride in STRIDES)
    return me, core, places


def greet(pos):
    me, core, places = pos
    barrier = pltpu.get_barrier_semaphore()
    pl.semaphore_signal(barrier, inc=1, device_id=(me + 1 - 2 * core,), device_id_type=MESH)
    for dim in range(3):
        for bit in (1, 2, 3):
            peer = me + (flip(places[dim], bit) - places[dim]) * STRIDES[dim]
            pl.semaphore_signal(barrier, inc=1, device_id=(peer,), device_id_type=MESH)
    pl.semaphore_wait(barrier, 10)


class SumAll:
    def __init__(self, acc, bufs, sems, pos, lanes):
        self.acc, self.bufs, self.sems, self.pos = acc, bufs, sems, pos
        third = lanes // 3 // 128 * 128
        self.groups = ((0, third), (third, third), (2 * third, lanes - 2 * third))

    def rows(self, start, size, lo, width):
        return self.acc.at[pl.ds(pl.multiple_of(start, 8), size), pl.ds(lo, width)]

    def copies(self, phase):
        me, core, places = self.pos
        send, recv = self.sems[:2]
        lanes = self.acc.shape[1]
        out = []

        def add(index, src, dst, peer):
            out.append(pltpu.make_async_remote_copy(src_ref=src, dst_ref=dst, send_sem=send.at[index], recv_sem=recv.at[index], device_id=(peer,), device_id_type=MESH))

        partner = me + 1 - 2 * core
        if phase == 0:
            add(0, self.rows((1 - core) * 128, 128, 0, lanes), self.bufs[0], partner)
            return out
        if phase == 6:
            mine = self.rows(core * 128, 128, 0, lanes)
            add(46, mine, mine, partner)
            return out
        for group, (lo, width) in enumerate(self.groups):
            first, second, third = ORDERS[group]
            top = core * 128
            block = top + places[first] * 32
            base = block + places[second] * 8
            dim = {1: first, 2: second, 3: third, 4: second, 5: first}[phase]
            for bit in (1, 2, 3):
                other = flip(places[dim], bit)
                peer = me + (other - places[dim]) * STRIDES[dim]
                index = 1 + (phase - 1) * 9 + group * 3 + bit - 1
                if phase == 1:
                    src, dst = self.rows(top + other * 32, 32, lo, width), self.bufs[1].at[bit - 1, :, pl.ds(lo, width)]
                elif phase == 2:
                    src, dst = self.rows(block + other * 8, 8, lo, width), self.bufs[2].at[bit - 1, :, pl.ds(lo, width)]
                elif phase == 3:
                    src, dst = self.rows(base, 8, lo, width), self.bufs[3].at[bit - 1, :, pl.ds(lo, width)]
                elif phase == 4:
                    src = dst = self.rows(base, 8, lo, width)
                else:
                    src = dst = self.rows(block, 32, lo, width)
                add(index, src, dst, peer)
        return out

    def start(self, phase):
        if phase == 6:
            pl.semaphore_wait(self.sems[2], 1)
        for copy in self.copies(phase):
            copy.start()

    def finish(self, phase):
        for copy in self.copies(phase):
            copy.wait()
        me, core, places = self.pos
        if phase == 0:
            pl.semaphore_signal(self.sems[2], inc=1, device_id=(me + 1 - 2 * core,), device_id_type=MESH)
            def add(k, carry):
                mine = self.rows(core * 128 + k * 8, 8, 0, self.acc.shape[1])
                mine[...] += self.bufs[0][pl.ds(pl.multiple_of(k * 8, 8), 8), :]
                return carry
            lax.fori_loop(0, 16, add, 0)
            return
        if phase > 3:
            return
        for group, (lo, width) in enumerate(self.groups):
            first, second, third = ORDERS[group]
            block = core * 128 + places[first] * 32
            for k in range(4 if phase == 1 else 1):
                got = [self.bufs[phase][bit, k * 8:k * 8 + 8, pl.ds(lo, width)] for bit in range(3)]
                mine = self.rows(block + k * 8 if phase == 1 else block + places[second] * 8, 8, lo, width)
                mine[...] = (mine[...] + got[0]) + (got[1] + got[2])

    def step(self, phase):
        if phase > 0:
            self.finish(phase - 1)
        if phase < 7:
            self.start(phase)


PLAN = {'e1_1': ('d1',),
 'pu1': ('d1',),
 'g1_2': ('u1', 'd1'),
 'sd0_1': ('d1', 'u1'),
 'e0_1': ('d1', 'u1', 'd0'),
 'e0_3': ('d1', 'u1'),
 'hats1': ('d0', 'd1', 'u1', 'u0', 'u1', 'd0', 'u1', 'u0', 'd0', 'hd1'),
 'qd1_1': ('u0',),
 'qd1_2': ('d0',),
 'qd1_3': ('u0',),
 'qu1': ('qd1', 'd0'),
 'qu1m': ('u0',),
 'hd0': ('d0',),
 'hu0': ('u0', 'qd1', 'qu1', 'u0'),
 'uu0_2': ('qd1',),
 'ud0_0': ('qd1', 'qu1'),
 'qd0': ('qu0',),
 'end': ('qd1',
         'qu1',
         'qd0',
         'qd1',
         'qu0',
         'qu1',
         'qd1',
         'qd0',
         'qu0',
         'qu1',
         'qd0',
         'qu0',
         'qu1',
         'qd0',
         'qu0',
         'qu1',
         'qd0',
         'qu0',
         'qd0',
         'qu0',
         'qd0')}
TILE = 512
LANES = 256
ROOT = math.sqrt(2.0 / math.pi)


def gelu(z):
    half = 0.5 * z
    return half + half * jnp.tanh(z * (ROOT + (ROOT * 0.044715) * (z * z)))


def gelu_slope(z):
    square = z * z
    t = jnp.tanh(z * (ROOT + (ROOT * 0.044715) * square))
    more = 1.0 + t
    return 0.5 * more + (more * z) * ((1.0 - t) * (0.5 * ROOT + (1.5 * ROOT * 0.044715) * square))


def tile_rows(i):
    return pl.ds(pl.multiple_of(i * TILE, TILE), TILE)


def step_kernel(axis, *refs):
    (x_hbm, dy_hbm, wu_hbm, wd_hbm, qu_hbm, qd_hbm, hat_u_hbm, hat_d_hbm, sum_u_hbm, sum_d_hbm,
     a0, z0, a1, z1, h1, g1, wu, wd, qu, qd, trans, stream_buf, pd1, pu1, pd0, pu0,
     stream_sem, load_sem, out_sem, *rest) = refs
    tiles = x_hbm.shape[0] // TILE
    bf16 = jnp.bfloat16
    f32 = jnp.float32
    channels = [rest[7 * k:7 * k + 7] for k in range(4)]

    def load(index, src, dst):
        return pltpu.make_async_copy(src, dst, load_sem.at[index])

    def tile_copy(src, i, slot):
        return pltpu.make_async_copy(src.at[tile_rows(i)], stream_buf.at[slot], stream_sem.at[slot])

    def loop(body, hooks=None):
        def run(i, carry):
            for when, hook in (hooks or {}).items():
                pl.when(i == when)(hook)
            body(i)
            return carry
        lax.fori_loop(0, tiles, run, 0)

    def streamed(src, following, body, hooks=None):
        def run(i):
            slot = lax.rem(i, 2)

            @pl.when(i + 1 < tiles)
            def _():
                tile_copy(src, i + 1, 1 - slot).start()
            tile_copy(src, i, slot).wait()
            body(i, stream_buf.at[slot])
        loop(run, hooks)
        if following is not None:
            tile_copy(following, 0, 0).start()

    tile_copy(x_hbm, 0, 0).start()
    load_wu0 = load(0, wu_hbm.at[0], wu)
    load_wd0 = load(1, wd_hbm.at[0], wd)
    load_qd1 = load(2, qd_hbm.at[1], qd)
    load_qu1 = load(3, qu_hbm.at[1], qu)
    load_wu1 = load(4, wu_hbm.at[1], wu)
    load_wd1 = load(5, wd_hbm.at[1], wd)
    load_wd0b = load(6, wd_hbm.at[0], wd)
    load_qd0 = load(7, qd_hbm.at[0], qd)
    load_qu0 = load(8, qu_hbm.at[0], qu)
    load_wu0.start()
    pos = position(axis)
    greet(pos)

    def reducer(acc, channel):
        return SumAll(acc, channels[channel][:4], channels[channel][4:], pos, acc.shape[1])

    places = {"d1": (pd1, 0), "u1": (pu1, 2), "d0": (pd0, 1), "u0": (pu0, 3), "qd1": (pu1, 2), "qu1": (pd1, 0), "qd0": (pu0, 3), "qu0": (pd0, 1)}
    sums = {name: reducer(*place) for name, place in places.items()}
    phases = dict.fromkeys(places, 0)
    spots = {"qd1": sum_d_hbm.at[1], "qu1": sum_u_hbm.at[1], "qd0": sum_d_hbm.at[0], "qu0": sum_u_hbm.at[0]}
    outs = {name: pltpu.make_async_copy(places[name][0], spot, out_sem.at[4 + k]) for k, (name, spot) in enumerate(spots.items())}

    def act(key):
        for name in PLAN.get(key, ()):
            if name == "hd1":
                normalise(pd1, wu, 0, 0, hat_d_hbm.at[1])
            else:
                advance(name)

    def advance(name):
        sums[name].step(phases[name])
        phases[name] += 1
        if phases[name] == 8 and name in outs:
            outs[name].start()

    def hooks(stage):
        return {i: functools.partial(act, stage + str(i)) for i in range(4) if PLAN.get(stage + str(i))}

    def up_rows(i, left, pre, post):
        for n in range(0, pre.shape[1], LANES):
            z = mat_nn(left, wu[:, n:n + LANES]).astype(bf16)
            pre[tile_rows(i), n:n + LANES] = z
            post[tile_rows(i), n:n + LANES] = gelu(z.astype(f32)).astype(bf16)

    def cot_rows(i, cot, pre):
        for n in range(0, pre.shape[1], LANES):
            c = mat_nt(cot, wd[n:n + LANES, :])
            z = pre[tile_rows(i), n:n + LANES].astype(f32)
            pre[tile_rows(i), n:n + LANES] = (gelu_slope(z) * c).astype(bf16)

    def put_trans(i, value):
        trans[:, tile_rows(i)] = value.T.astype(bf16)

    def full_product(acc, right, key=None):
        for n in range(0, acc.shape[1], 256):
            if key and n == acc.shape[1] // 2:
                act(key)
            acc[:, n:n + 256] = mat_nn(trans[...], right[:, n:n + 256])

    def add_product(i, acc, left, right):
        @pl.when(i == 0)
        def _():
            acc[...] = jnp.zeros_like(acc)
        for n in range(0, acc.shape[1], 256):
            acc[:, n:n + 256] += mat_nn(left, right[:, n:n + 256])

    def normalise(acc, out, row, index, dst):
        def run(k, carry):
            rows = pl.ds(pl.multiple_of(k * 32, 32), 32)
            p = acc[rows, :]
            out[pl.ds(pl.multiple_of(row + k * 32, 32), 32), :] = (p / jnp.sqrt(jnp.sum(p * p, axis=1, keepdims=True))).astype(bf16)
            return carry
        lax.fori_loop(0, 8, run, 0)
        pltpu.make_async_copy(out.at[row:row + 256], dst, out_sem.at[index]).start()

    def z0_stage(i, x_tile):
        up_rows(i, x_tile[...], z0, a0)

    load_wu0.wait()
    load_wd0.start()
    load_qd1.start()
    load_qu1.start()
    streamed(x_hbm, x_hbm, z0_stage)
    load_wu1.start()
    load_wd0.wait()

    def h1_stage(i, x_tile):
        for n in range(0, h1.shape[1], 256):
            h1[tile_rows(i), n:n + 256] = (x_tile[:, n:n + 256].astype(f32) + mat_nn(a0[tile_rows(i), :], wd[:, n:n + 256])).astype(bf16)
    streamed(x_hbm, dy_hbm, h1_stage)
    load_wd1.start()
    load_wu1.wait()
    loop(lambda i: up_rows(i, h1[tile_rows(i), :], z1, a1))
    load_qd1.wait()

    def sd1_stage(i, dy_tile):
        put_trans(i, mat_nn(dy_tile[...], qd[...]))
    streamed(dy_hbm, dy_hbm, sd1_stage)
    load_qd0.start()
    full_product(pd1, a1)
    advance("d1")
    load_wd1.wait()
    load_qu1.wait()

    def e1_stage(i, dy_tile):
        cot_rows(i, dy_tile[...], z1)
        put_trans(i, mat_nn(z1[tile_rows(i), :], qu[...]))
    streamed(dy_hbm, dy_hbm, e1_stage, hooks("e1_"))
    load_wd0b.start()
    load_qu0.start()
    act("pu1")
    full_product(pu1, h1)
    advance("u1")

    def g1_stage(i, dy_tile):
        for n in range(0, g1.shape[1], 256):
            g1[tile_rows(i), n:n + 256] = (dy_tile[:, n:n + 256].astype(f32) + mat_nt(z1[tile_rows(i), :], wu[n:n + 256, :])).astype(bf16)
    streamed(dy_hbm, x_hbm, g1_stage, hooks("g1_"))
    load_qd0.wait()
    loop(lambda i: put_trans(i, mat_nn(g1[tile_rows(i), :], qd[...])), hooks("sd0_"))
    act("pd0")
    full_product(pd0, a0, "pd0m")
    advance("d0")
    load_wd0b.wait()
    load_qu0.wait()

    def e0_stage(i, x_tile):
        cot_rows(i, g1[tile_rows(i), :], z0)
        sketch = mat_nn(z0[tile_rows(i), :], qu[...]).T.astype(bf16)
        add_product(i, pu0, sketch, x_tile)
    streamed(x_hbm, dy_hbm, e0_stage, hooks("e0_"))
    advance("u0")
    act("hats1")
    normalise(pu1, wd, 0, 1, hat_u_hbm.at[1])

    def qd1_stage(i, dy_tile):
        back = mat_nt(a1[tile_rows(i), :], wu[0:256, :]).T.astype(bf16)
        add_product(i, pu1, back, dy_tile)
    streamed(dy_hbm, x_hbm, qd1_stage, hooks("qd1_"))
    advance("qd1")
    loop(lambda i: put_trans(i, mat_nt(h1[tile_rows(i), :], wd[0:256, :])), hooks("uu1_"))
    act("qu1")
    full_product(pd1, z1, "qu1m")
    advance("qu1")
    act("hd0")
    normalise(pd0, wu, 256, 2, hat_d_hbm.at[0])
    act("hu0")
    normalise(pu0, wd, 256, 3, hat_u_hbm.at[0])

    def uu0_stage(i, x_tile):
        put_trans(i, mat_nt(x_tile[...], wd[256:512, :]))
    streamed(x_hbm, None, uu0_stage, hooks("uu0_"))
    act("qu0")
    full_product(pd0, z0, "qu0m")
    advance("qu0")
    loop(lambda i: put_trans(i, mat_nt(a0[tile_rows(i), :], wu[256:512, :])), hooks("ud0_"))
    act("qd0")
    full_product(pu0, g1)
    advance("qd0")
    act("end")
    assert set(phases.values()) == {8}
    hats = [(wu, 0, hat_d_hbm.at[1]), (wd, 0, hat_u_hbm.at[1]), (wu, 256, hat_d_hbm.at[0]), (wd, 256, hat_u_hbm.at[0])]
    for k, (src, row, dst) in enumerate(hats):
        pltpu.make_async_copy(src.at[row:row + 256], dst, out_sem.at[k]).wait()
    for copy in outs.values():
        copy.wait()


def sum_scratch(lanes):
    return [pltpu.VMEM((128, lanes), jnp.float32), pltpu.VMEM((3, 32, lanes), jnp.float32), pltpu.VMEM((3, 8, lanes), jnp.float32), pltpu.VMEM((3, 8, lanes), jnp.float32), pltpu.SemaphoreType.DMA((COPIES,)), pltpu.SemaphoreType.DMA((COPIES,)), pltpu.SemaphoreType.REGULAR]


def power_sums(axis, tok_rows, grad_rows, w_up, w_down, q_up, q_down):
    tokens, model = tok_rows.shape
    layers, _, wide = w_up.shape
    rank = q_up.shape[-1]
    bf16, f32 = jnp.bfloat16, jnp.float32
    scratch = [pltpu.VMEM((tokens, wide), bf16)] * 4 + [pltpu.VMEM((tokens, model), bf16)] * 2
    scratch += [pltpu.VMEM((model, wide), bf16), pltpu.VMEM((wide, model), bf16), pltpu.VMEM((wide, rank), bf16), pltpu.VMEM((model, rank), bf16)]
    scratch += [pltpu.VMEM((rank, tokens), bf16), pltpu.VMEM((2, TILE, model), bf16)]
    scratch += [pltpu.VMEM((rank, lanes), f32) for lanes in (wide, model, wide, model)]
    scratch += [pltpu.SemaphoreType.DMA((2,)), pltpu.SemaphoreType.DMA((9,)), pltpu.SemaphoreType.DMA((8,))]
    for lanes in (wide, wide, model, model):
        scratch += sum_scratch(lanes)
    return pl.pallas_call(
        functools.partial(step_kernel, axis),
        out_shape=[jax.ShapeDtypeStruct((layers, rank, model), bf16), jax.ShapeDtypeStruct((layers, rank, wide), bf16), jax.ShapeDtypeStruct((layers, rank, wide), f32), jax.ShapeDtypeStruct((layers, rank, model), f32)],
        in_specs=[pl.BlockSpec(memory_space=pl.ANY)] * 6,
        out_specs=[pl.BlockSpec(memory_space=pl.ANY)] * 4,
        scratch_shapes=scratch,
        compiler_params=pltpu.CompilerParams(collective_id=0, has_side_effects=True, vmem_limit_bytes=67043328),
        name="power_sums",
    )(tok_rows, grad_rows, w_up, w_down, q_up, q_down)


def update_kernel(step_size, hat_u_hbm, hat_d_hbm, sum_u_hbm, sum_d_hbm, wu_hbm, wd_hbm, wu_out, wd_out, fac_u_out, fac_d_out,
                  hat_u, hat_d, sum_u, sum_d, wu, wd, turn_u, turn_d, small_sem, w_sem, out_sem, fac_sem):
    layers, model, wide = wu.shape
    rank = hat_u.shape[1]
    bf16, f32 = jnp.bfloat16, jnp.float32
    order = tuple(reversed(range(layers)))
    chunk_u, chunk_d = model // 3, wide // 4

    def small(l, k, src, dst):
        return pltpu.make_async_copy(src.at[l], dst.at[l], small_sem.at[l, k])

    def part(l, k):
        if k < 3:
            return wu_hbm.at[l, k * chunk_u:(k + 1) * chunk_u], wu.at[l, k * chunk_u:(k + 1) * chunk_u], wu_out.at[l, k * chunk_u:(k + 1) * chunk_u]
        rows = slice((k - 3) * chunk_d, (k - 2) * chunk_d)
        return wd_hbm.at[l, rows], wd.at[l, rows], wd_out.at[l, rows]

    def smalls(l, half):
        pairs = ((sum_d_hbm, sum_d), (hat_d_hbm, hat_d)) if half else ((sum_u_hbm, sum_u), (hat_u_hbm, hat_u))
        return [small(l, 2 * half + k, src, dst) for k, (src, dst) in enumerate(pairs)]

    def load(l, k):
        src, dst, _ = part(l, k)
        return pltpu.make_async_copy(src, dst, w_sem.at[l, k])

    def store(l, k):
        _, src, dst = part(l, k)
        return pltpu.make_async_copy(src, dst, out_sem.at[l, k])

    def store_fac(l, half):
        return pltpu.make_async_copy((turn_d if half else turn_u).at[l], (fac_d_out if half else fac_u_out).at[l], fac_sem.at[l, half])

    for l in order:
        for copy in smalls(l, 0) + [load(l, k) for k in range(3)] + smalls(l, 1) + [load(l, k) for k in range(3, 7)]:
            copy.start()

    def run(index, carry):
        l = layers - 1 - index
        for half, (total, hat, w, turn, width, count, lanes) in enumerate(((sum_u, hat_u, wu, turn_u, chunk_u, 3, 512), (sum_d, hat_d, wd, turn_d, chunk_d, 4, 384))):
            for copy in smalls(l, half):
                copy.wait()
            for n in range(0, total.shape[2], lanes):
                turn[l, n:n + lanes, :] = total[l, :, n:n + lanes].T
            store_fac(l, half).start()
            for k in range(count):
                load(l, 3 * half + k).wait()
                rows = slice(k * width, (k + 1) * width)
                for n in range(0, w.shape[2], lanes):
                    step = step_size * mat_tn(hat[l, :, rows], total[l, :, n:n + lanes].astype(bf16))
                    w[l, rows, n:n + lanes] = (w[l, rows, n:n + lanes].astype(f32) - step).astype(bf16)
                store(l, 3 * half + k).start()
        return carry

    lax.fori_loop(0, layers, run, 0)
    for l in order:
        for k in range(7):
            store(l, k).wait()
        for half in range(2):
            store_fac(l, half).wait()


def update(step_size, hat_u, hat_d, sum_u, sum_d, w_up, w_down):
    layers, model, wide = w_up.shape
    rank = hat_u.shape[1]
    bf16, f32 = jnp.bfloat16, jnp.float32
    return pl.pallas_call(
        functools.partial(update_kernel, step_size),
        in_specs=[pl.BlockSpec(memory_space=pl.ANY)] * 6,
        out_specs=[pl.BlockSpec(memory_space=pl.ANY)] * 4,
        out_shape=[jax.ShapeDtypeStruct((layers, model, wide), bf16), jax.ShapeDtypeStruct((layers, wide, model), bf16), jax.ShapeDtypeStruct((layers, wide, rank), f32), jax.ShapeDtypeStruct((layers, model, rank), f32)],
        scratch_shapes=[pltpu.VMEM(hat_u.shape, bf16), pltpu.VMEM(hat_d.shape, bf16), pltpu.VMEM(sum_u.shape, f32), pltpu.VMEM(sum_d.shape, f32), pltpu.VMEM(w_up.shape, bf16), pltpu.VMEM(w_down.shape, bf16), pltpu.VMEM((layers, wide, rank), f32), pltpu.VMEM((layers, model, rank), f32), pltpu.SemaphoreType.DMA((layers, 4)), pltpu.SemaphoreType.DMA((layers, 7)), pltpu.SemaphoreType.DMA((layers, 7)), pltpu.SemaphoreType.DMA((layers, 2))],
        compiler_params=pltpu.CompilerParams(vmem_limit_bytes=60 * 2**20),
        name="update",
    )(hat_u, hat_d, sum_u, sum_d, w_up, w_down)


def solution(mesh):
    axis = mesh.axis_names[0]

    def local_step(tok_rows, grad_rows, w_up, w_down, q_up, q_down):
        step_size = 0.4 / math.sqrt(q_up.shape[-1])
        hat_u, hat_d, sum_u, sum_d = power_sums(axis, tok_rows, grad_rows, w_up, w_down, q_up, q_down)
        return tuple(update(step_size, hat_u, hat_d, sum_u, sum_d, w_up, w_down))

    row_spec = P(axis, None)
    return jax.shard_map(local_step, mesh=mesh, in_specs=(row_spec, row_spec, P(), P(), P(), P()), out_specs=(P(), P(), P(), P()), check_vma=False)
```
